128 devices in a mesh: grp: 2 (over x_lo), wide: 64 (over z, x_hi, y, core).
Axes of the slice: x: 4 (x_hi: 2, x_lo: 2; x = x_hi * 2 + x_lo), y: 4, z: 4, core: 2. Of those that a mesh axis runs over, the one named last changes fastest.
Arguments:
- x_pool: bfloat16 [65536, 7168], P(('grp', 'wide')), may hold values from -6 to 6
- token_ids: int32 [16384], P(('grp', 'wide')), may hold values from 0 to 65535, as said below
- cotangent: bfloat16 [16384, 7168], P(('grp', 'wide')), may hold values from -6 to 6
- gate_up: bfloat16 [2, 1024, 7168], P(None, 'wide', 'grp'), may hold values from -0.0625 to 0.0625
- down_weight: bfloat16 [1024, 7168], P('wide', 'grp'), may hold values from -0.1875 to 0.1875
- loss_exponent: int32 [1], replicated, may hold values from 3 to 9
Outputs:
- grad_gate_up: bfloat16 [2, 1024, 7168], P(None, 'wide', 'grp')
- grad_down: bfloat16 [1024, 7168], P('wide', 'grp')
The draws below stay inside these ranges and needn't reach their ends.
Inputs may be any that keep to these rules, and one draw needn't show every extreme that they name: The 128 ids in aligned block b of token_ids name rows b * 512 to (b + 1) * 512 - 1 of x_pool.
All inputs are finite; a program needn't handle non-finite values.
Results may differ from the reference program's by a relative error of at most 0.014.
Values may be sent and summed in bfloat16 or wider, within the bound.
A program may use at most 192 MiB of HBM per device.

```python
import jax
import jax.numpy as jnp
import numpy as np

D = 7168
F = 1024
BLOCKS = 8
TOK_DEV = 128
POOL_DEV = 512
TOKENS = 16384
POOL = 65536
N_GRP = 2
N_WIDE = 64


def draw_token_ids(key, part):
    offsets = jnp.arange(TOKENS, dtype=jnp.int32) // TOK_DEV * POOL_DEV
    return offsets + jax.random.randint(key, (TOKENS,), 0, POOL_DEV, dtype=jnp.int32)


def shard_levels(key, shape, pieces, smallest, top_value):
    level, own = 1.0, jax.random.fold_in(key, 6)
    for dim, shards_of in pieces:
        heights = jnp.exp(jax.random.uniform(jax.random.fold_in(own, dim), (shards_of,), jnp.float32, smallest / len(pieces), top_value / len(pieces)))
        level = level * jnp.repeat(heights, shape[dim] // shards_of).reshape([-1 if axis == dim else 1 for axis in range(len(shape))])
    return level


def scatter_about(key, extent, width, limit, cuts=(), held_as=jnp.bfloat16):
    gain = shard_levels(key, extent, cuts, -0.22, 0.18) if cuts else 1.0
    drawn = jax.random.normal(key, extent, jnp.float32) * width * gain
    return jnp.minimum(jnp.maximum(drawn, -limit), limit).astype(held_as)


def setup_inputs(seed: int = 0) -> dict:
    key_of = jax.random.split(jax.random.key(seed), 7)
    return {
        "x_pool": scatter_about(key_of[0], (POOL, D), 1.0, 6.0, ((0, 128),)),
        "token_ids": draw_token_ids(jax.random.fold_in(key_of[6], 71), 0),
        "cotangent": scatter_about(key_of[2], (TOKENS, D), 1.0, 6.0, ((0, 128),)),
        "gate_up": scatter_about(key_of[3], (2, F, D), D ** -0.5, 0.0625, ((1, 64), (2, 2))),
        "down_weight": scatter_about(key_of[4], (F, D), F ** -0.5, 0.1875, ((0, 64), (1, 2))),
        "loss_exponent": jax.random.randint(key_of[5], (1,), 3, 10).astype(jnp.int32),
    }


def unscale_of(loss_exponent):
    levels = jnp.arange(16, dtype=jnp.int32)
    powers = jnp.asarray(np.power(0.5, np.arange(16)), dtype=jnp.float32)
    return jnp.sum(jnp.where(levels == loss_exponent[0], powers, jnp.float32(0.0)))


def reference(x_pool, token_ids, cotangent, gate_up, down_weight, loss_exponent):
    picked = jnp.take(x_pool, token_ids, axis=0)
    unscale = unscale_of(loss_exponent)
    gate_act = jnp.dot(picked, gate_up[0].T, preferred_element_type=jnp.float32)
    up_act = jnp.dot(picked, gate_up[1].T, preferred_element_type=jnp.float32)
    delta_hidden = unscale * jnp.dot(cotangent, down_weight.T, preferred_element_type=jnp.float32)
    sigmoid_gate = jax.nn.sigmoid(gate_act)
    hidden = (gate_act * sigmoid_gate * up_act).astype(jnp.bfloat16)
    delta_gate = (delta_hidden * up_act * sigmoid_gate * (1.0 + gate_act * (1.0 - sigmoid_gate))).astype(jnp.bfloat16)
    delta_up = (delta_hidden * gate_act * sigmoid_gate).astype(jnp.bfloat16)
    set_count = N_GRP * (N_WIDE // BLOCKS)
    set_rows = TOKENS // set_count
    total_gate = jnp.zeros((F, D), jnp.float32)
    total_up = jnp.zeros((F, D), jnp.float32)
    total_down = jnp.zeros((F, D), jnp.float32)
    for set_index in range(set_count):
        lower = set_index * set_rows
        upper = lower + set_rows
        rows_in = picked[lower:upper]
        part_gate = jnp.dot(delta_gate[lower:upper].T, rows_in, preferred_element_type=jnp.float32)
        part_up = jnp.dot(delta_up[lower:upper].T, rows_in, preferred_element_type=jnp.float32)
        part_down = unscale * jnp.dot(hidden[lower:upper].T, cotangent[lower:upper], preferred_element_type=jnp.float32)
        total_gate = total_gate + part_gate.astype(jnp.bfloat16).astype(jnp.float32)
        total_up = total_up + part_up.astype(jnp.bfloat16).astype(jnp.float32)
        total_down = total_down + part_down.astype(jnp.bfloat16).astype(jnp.float32)
    grad_gate_up = jnp.stack([total_gate, total_up]).astype(jnp.bfloat16)
    grad_down = total_down.astype(jnp.bfloat16)
    return grad_gate_up, grad_down
```

```python
import functools

import jax
import jax.numpy as jnp
from jax import lax
from jax.experimental import pallas as pl
from jax.experimental.pallas import tpu as pltpu
from jax.sharding import PartitionSpec as P

MESH = pl.DeviceIdType.MESH
BF16 = jnp.bfloat16
F32 = jnp.float32
COPIES = 128
LOCALS = 16


def dot_nt(a, b):
    return lax.dot_general(a, b, (((1,), (1,)), ((), ())), preferred_element_type=F32)


def dot_nn(a, b):
    return lax.dot_general(a, b, (((1,), (0,)), ((), ())), preferred_element_type=F32)


class Wire:
    def __init__(self, send_sems, recv_sems):
        self.send_sems, self.recv_sems = send_sems, recv_sems
        self.count = 0
        self.sent = []

    def send(self, src, dst, device):
        copy = pltpu.make_async_remote_copy(
            src_ref=src,
            dst_ref=dst,
            send_sem=self.send_sems.at[self.count],
            recv_sem=self.recv_sems.at[self.count],
            device_id=device,
            device_id_type=MESH,
        )
        self.count += 1
        copy.start()
        self.sent.append(copy)
        return copy

    def drain(self):
        for copy in self.sent:
            copy.wait_send()


def kernel(
    pool, ids, cot, gate_up, down, exponent,
    out_pair, out_down,
    tok_x, tok_c, via_x, via_c, picked, pool_q, weights,
    part, part_own, r1p, r1m, r2p, r2m, deltas, grads,
    ra1p, ra1m, ra2p, ra2m, sum_a, ya1p, ya1m, ya2p, ya2m,
    yb1p, yb1m, yb2p, yb2m, sum_b, zb1p, zb1m, zb2p, zb2m,
    final, crossed, send_sems, recv_sems, local_sems,
):
    tokens, width = cot.shape
    quarter = width // 4
    half = quarter // 2
    own_rows = down.shape[0]
    pair_rows = 2 * own_rows
    chunk_rows = 4 * pair_rows
    chip_tokens = 2 * tokens
    pool_rows = pool.shape[0]
    tile = 256 if quarter % 256 == 0 else quarter

    x_lo = lax.axis_index("grp")
    wide = lax.axis_index("wide")
    z = lax.div(wide, 16)
    x_hi = lax.rem(lax.div(wide, 8), 2)
    y = lax.rem(lax.div(wide, 2), 4)
    core = lax.rem(wide, 2)
    x = 2 * x_hi + x_lo
    device_index = x_lo * 64 + wide

    def shift(v, by):
        return lax.rem(v + (by % 4), 4)

    def device(xx, yy, zz, cc):
        return (lax.rem(xx, 2), zz * 16 + lax.div(xx, 2) * 8 + yy * 2 + cc)

    xn, xf, xb = shift(x, 1), shift(x, 2), shift(x, -1)
    yn, yf, yb = shift(y, 1), shift(y, 2), shift(y, -1)
    zn, zf, zb = shift(z, 1), shift(z, 2), shift(z, -1)
    x_next, x_far, x_back = (device(v, y, z, core) for v in (xn, xf, xb))
    y_next, y_back = (device(x, v, z, core) for v in (yn, yb))
    z_next, z_back = (device(x, y, v, core) for v in (zn, zb))
    partner = device(x, y, z, 1 - core)

    def feature_quarter(xx):
        return 2 * lax.rem(xx, 2) + lax.div(xx, 2)

    def q_cols(xx):
        return pl.ds(pl.multiple_of(feature_quarter(xx) * quarter, quarter), quarter)

    def slot(xx, cc):
        return pl.ds(pl.multiple_of((2 * xx + cc) * tokens, tokens), tokens)

    def chip_slot(xx):
        return pl.ds(pl.multiple_of(xx * chip_tokens, chip_tokens), chip_tokens)

    def rows_of(yy):
        return pl.ds(pl.multiple_of(yy * pair_rows, pair_rows), pair_rows)

    def low_rows_of(yy):
        return pl.ds(pl.multiple_of(yy * pair_rows, own_rows), own_rows)

    def high_rows_of(yy):
        return pl.ds(pl.multiple_of(yy * pair_rows + own_rows, own_rows), own_rows)

    def owner_rows(xh):
        return pl.ds(pl.multiple_of(y * pair_rows + xh * own_rows, own_rows), own_rows)

    cols_a = pl.ds(0, half)
    cols_b = pl.ds(half, half)
    all_p = pl.ds(0, 3)
    wire = Wire(send_sems, recv_sems)
    locals_used = [0]

    def fetch(src, dst):
        copy = pltpu.make_async_copy(src, dst, local_sems.at[locals_used[0]])
        locals_used[0] += 1
        copy.start()
        return copy

    far_pool = fetch(pool.at[:, q_cols(xf)], pool_q.at[0])

    barrier = pltpu.get_barrier_semaphore()
    for peer in (x_next, x_back, x_far, y_next, y_back, z_next, z_back, partner):
        pl.semaphore_signal(barrier, inc=1, device_id=peer, device_id_type=MESH)
    pl.semaphore_wait(barrier, 8)

    x_hi_cols = pl.ds(pl.multiple_of(x_hi * quarter, quarter), quarter)
    other_cols = pl.ds(pl.multiple_of((1 - x_hi) * quarter, quarter), quarter)
    wx_pair = wire.send(
        gate_up.at[:, :, other_cols], weights.at[z, pl.ds(0, 2), owner_rows(x_hi), :], x_far
    )
    wx_down = wire.send(down.at[:, other_cols], weights.at[z, 2, owner_rows(x_hi), :], x_far)
    w_pair = fetch(gate_up.at[:, :, x_hi_cols], weights.at[z, pl.ds(0, 2), owner_rows(x_hi), :])
    w_down = fetch(down.at[:, x_hi_cols], weights.at[z, 2, owner_rows(x_hi), :])

    c_via = wire.send(cot.at[:, q_cols(xf)], via_c, x_back)
    c_back = wire.send(cot.at[:, q_cols(xb)], tok_c.at[slot(x, core), :], x_back)
    c_own = fetch(cot.at[:, q_cols(x)], tok_c.at[slot(x, core), :])
    next_pool = fetch(pool.at[:, q_cols(xn)], pool_q.at[1])
    back_pool = fetch(pool.at[:, q_cols(xb)], pool_q.at[2])
    own_pool = fetch(pool.at[:, q_cols(x)], pool_q.at[3])

    local_ids = ids[...] - device_index * pool_rows
    row_ids = lax.broadcasted_iota(jnp.int32, (pool_rows, tokens), 0)
    chosen = jnp.where(row_ids == local_ids, 1.0, 0.0).astype(F32).T.astype(BF16)

    def pick(index, target, row_slot):
        def step(n, carry):
            cols = pl.ds(pl.multiple_of(n * tile, tile), tile)
            target[row_slot, cols] = dot_nn(chosen, pool_q[index, :, cols]).astype(BF16)
            return carry

        lax.fori_loop(0, quarter // tile, step, 0)

    every = pl.ds(0, tokens)
    far_pool.wait()
    pick(0, picked.at[0], every)
    x_via = wire.send(picked.at[0], via_x, x_next)
    c_next = wire.send(cot.at[:, q_cols(xn)], tok_c.at[slot(x, core), :], x_next)

    w_pair.wait()
    w_down.wait()
    wx_pair.wait_recv()
    wx_down.wait_recv()

    def w_block(zz, rows, cols):
        return weights.at[zz, all_p, rows, cols]

    def same(view, device_):
        return wire.send(view, view, device_)

    a_next = same(w_block(z, rows_of(y), cols_a), y_next)
    a_back = same(w_block(z, rows_of(y), cols_a), y_back)
    b_next = same(w_block(z, rows_of(y), cols_b), z_next)
    b_back = same(w_block(z, rows_of(y), cols_b), z_back)

    own_pool.wait()
    pick(3, tok_x, slot(x, core))
    dd_own_x = same(tok_x.at[slot(x, core), :], partner)
    c_own.wait()
    dd_own_c = same(tok_c.at[slot(x, core), :], partner)
    next_pool.wait()
    pick(1, picked.at[1], every)
    back_pool.wait()
    pick(2, picked.at[2], every)

    a_next.wait_recv()
    a_on = same(w_block(z, low_rows_of(yb), cols_a), y_next)
    a_back.wait_recv()
    a_off = same(w_block(z, high_rows_of(yn), cols_a), y_back)
    b_next.wait_recv()
    b_on = same(w_block(zb, low_rows_of(y), cols_b), z_next)
    b_back.wait_recv()
    b_off = same(w_block(zn, high_rows_of(y), cols_b), z_back)

    a_on.wait_recv()
    a_off.wait_recv()
    every_row = pl.ds(0, chunk_rows)
    lower, upper = pl.ds(0, chunk_rows // 2), pl.ds(chunk_rows // 2, chunk_rows // 2)
    a2_next = same(w_block(z, every_row, cols_a), z_next)
    a2_back = same(w_block(z, every_row, cols_a), z_back)
    b_on.wait_recv()
    b_off.wait_recv()
    b2_next = same(w_block(pl.ds(0, 4), rows_of(y), cols_b), y_next)
    b2_back = same(w_block(pl.ds(0, 4), rows_of(y), cols_b), y_back)

    c_via.wait_recv()
    c_pass = wire.send(via_c, tok_c.at[slot(xn, core), :], x_back)
    x_back_copy = wire.send(picked.at[2], tok_x.at[slot(x, core), :], x_back)
    x_via.wait_recv()
    x_pass = wire.send(via_x, tok_x.at[slot(xb, core), :], x_next)
    x_next_copy = wire.send(picked.at[1], tok_x.at[slot(x, core), :], x_next)

    c_back.wait_recv()
    dd_c_n = same(tok_c.at[slot(xn, core), :], partner)
    c_next.wait_recv()
    dd_c_b = same(tok_c.at[slot(xb, core), :], partner)

    a2_next.wait_recv()
    a2_on = same(w_block(zb, lower, cols_a), z_next)
    a2_back.wait_recv()
    a2_off = same(w_block(zn, upper, cols_a), z_back)
    b2_next.wait_recv()
    b2_on = same(w_block(pl.ds(0, 2), rows_of(yb), cols_b), y_next)
    b2_back.wait_recv()
    b2_off = same(w_block(pl.ds(2, 2), rows_of(yn), cols_b), y_back)

    c_pass.wait_recv()
    dd_c_f = same(tok_c.at[slot(xf, core), :], partner)
    x_pass.wait_recv()
    dd_x_f = same(tok_x.at[slot(xf, core), :], partner)

    for copy in (a2_on, a2_off, b2_on, b2_off):
        copy.wait_recv()

    def forward(xx, target):
        def step(j, carry):
            tx = tok_x[chip_slot(xx), :]
            for h in range(2):
                pair = weights[2 * j + h, 0:2].reshape(2 * chunk_rows, quarter)
                target[2 * j + h, :, 0 : 2 * chunk_rows] = dot_nt(tx, pair).astype(target.dtype)
            tc = tok_c[chip_slot(xx), :]
            both = weights[pl.ds(2 * j, 2), 2].reshape(2 * chunk_rows, quarter)
            back = dot_nt(tc, both).astype(target.dtype)
            target[2 * j, :, 2 * chunk_rows :] = back[:, :chunk_rows]
            target[2 * j + 1, :, 2 * chunk_rows :] = back[:, chunk_rows:]
            return carry

        lax.fori_loop(0, 2, step, 0)

    first, second = pl.ds(0, tokens), pl.ds(tokens, tokens)
    dd_c_f.wait_recv()
    dd_x_f.wait_recv()
    forward(xf, part.at[xf])
    order = (zf, zn, zb, z)
    rs1 = []
    for zz in order:
        rs1.append(
            (
                wire.send(part.at[xf, zz, first, :], r1p.at[zz], x_next),
                wire.send(part.at[xf, zz, second, :], r1m.at[zz], x_back),
            )
        )
    dd_own_x.wait_recv()
    dd_own_c.wait_recv()
    forward(x, part_own)

    x_back_copy.wait_recv()
    dd_x_n = same(tok_x.at[slot(xn, core), :], partner)
    x_next_copy.wait_recv()
    dd_x_b = same(tok_x.at[slot(xb, core), :], partner)
    dd_c_n.wait_recv()
    dd_x_n.wait_recv()
    forward(xn, part.at[xn])
    dd_c_b.wait_recv()
    dd_x_b.wait_recv()
    forward(xb, part.at[xb])

    def add_into(ref, *others):
        total = ref[...].astype(F32)
        for other in others:
            total = total + other[...].astype(F32)
        ref[...] = total.astype(ref.dtype)

    rs2 = []
    for k, zz in enumerate(order):
        rs1[k][0].wait_recv()
        add_into(part.at[xn, zz, first, :], r1p.at[zz])
        fwd = wire.send(part.at[xn, zz], r2p.at[zz], x_next)
        rs1[k][1].wait_recv()
        add_into(part.at[xb, zz, second, :], r1m.at[zz])
        rs2.append((fwd, wire.send(part.at[xb, zz], r2m.at[zz], x_back)))

    level = exponent[0]
    unscale = jnp.float32(0.0)
    for power in range(16):
        unscale = jnp.where(level == power, jnp.float32(0.5**power), unscale)

    def own_lanes(xx):
        return pl.ds(pl.multiple_of(xx * chip_tokens, chip_tokens), chip_tokens)

    def low_lanes(xx):
        return pl.ds(pl.multiple_of(xx * chip_tokens, tokens), tokens)

    def high_lanes(xx):
        return pl.ds(pl.multiple_of(xx * chip_tokens + tokens, tokens), tokens)

    every_unit = pl.ds(0, chunk_rows)
    ag = []
    for k, zz in enumerate(order):
        rs2[k][0].wait_recv()
        rs2[k][1].wait_recv()
        total = part_own[zz] + r2p[zz].astype(F32) + r2m[zz].astype(F32)
        gate = total[:, :chunk_rows]
        up = total[:, chunk_rows : 2 * chunk_rows]
        delta = unscale * total[:, 2 * chunk_rows :]
        sig = 1.0 / (1.0 + jnp.exp(-gate))
        hidden = gate * sig * up
        delta_gate = delta * up * sig * (1.0 + gate * (1.0 - sig))
        delta_up = delta * gate * sig
        deltas[zz, 0, :, own_lanes(x)] = delta_gate.T.astype(BF16)
        deltas[zz, 1, :, own_lanes(x)] = delta_up.T.astype(BF16)
        deltas[zz, 2, :, own_lanes(x)] = hidden.T.astype(BF16)
        mine = deltas.at[zz, all_p, every_unit, own_lanes(x)]
        ag.append((same(mine, x_next), same(mine, x_back)))

    passed = []

    def pass_on(k):
        zz = order[k]
        ag[k][0].wait_recv()
        on = same(deltas.at[zz, all_p, every_unit, low_lanes(xb)], x_next)
        ag[k][1].wait_recv()
        passed.append((on, same(deltas.at[zz, all_p, every_unit, high_lanes(xn)], x_back)))

    def gradient(k):
        zz = order[k]
        passed[k][0].wait_recv()
        passed[k][1].wait_recv()

        def step(n, carry):
            cols = pl.ds(pl.multiple_of(n * tile, tile), tile)
            pair = deltas[zz, 0:2].reshape(2 * chunk_rows, 4 * chip_tokens)
            out = dot_nn(pair, tok_x[:, cols]).astype(BF16)
            grads[zz, 0, :, cols] = out[:chunk_rows]
            grads[zz, 1, :, cols] = out[chunk_rows:]
            down_part = unscale * dot_nn(deltas[zz, 2], tok_c[:, cols])
            grads[zz, 2, :, cols] = down_part.astype(BF16)
            return carry

        lax.fori_loop(0, quarter // tile, step, 0)

    def g_block(zz, rows, cols):
        return grads.at[zz, all_p, rows, cols]

    def add3(out, *terms):
        for p in range(3):
            total = terms[0][p].astype(F32)
            for term in terms[1:]:
                total = total + term[p].astype(F32)
            out[p] = total.astype(out.dtype)

    yb1, yb2 = {}, {}

    def b_first(k):
        zz = order[k]
        yb1[k] = (
            wire.send(g_block(zz, low_rows_of(yf), cols_b), yb1p.at[zz], y_next),
            wire.send(g_block(zz, high_rows_of(yf), cols_b), yb1m.at[zz], y_back),
        )

    def b_second(k):
        zz = order[k]
        yb1[k][0].wait_recv()
        view = g_block(zz, low_rows_of(yn), cols_b)
        add3(view, view, yb1p.at[zz])
        on = wire.send(g_block(zz, rows_of(yn), cols_b), yb2p.at[zz], y_next)
        yb1[k][1].wait_recv()
        view = g_block(zz, high_rows_of(yb), cols_b)
        add3(view, view, yb1m.at[zz])
        yb2[k] = (on, wire.send(g_block(zz, rows_of(yb), cols_b), yb2m.at[zz], y_back))

    def b_sum(k, *more):
        zz = order[k]
        yb2[k][0].wait_recv()
        yb2[k][1].wait_recv()
        add3(sum_b.at[zz], g_block(zz, rows_of(y), cols_b), yb2p.at[zz], yb2m.at[zz])

    own_low, own_high = pl.ds(0, own_rows), pl.ds(own_rows, own_rows)

    def s_block(zz, rows):
        return sum_b.at[zz, all_p, rows, :]

    pass_on(0)
    pass_on(1)
    gradient(0)
    za1 = (
        wire.send(g_block(zf, lower, cols_a), ra1p, z_next),
        wire.send(g_block(zf, upper, cols_a), ra1m, z_back),
    )
    b_first(0)
    pass_on(2)

    gradient(1)
    za1[0].wait_recv()
    view = g_block(zn, lower, cols_a)
    add3(view, view, ra1p)
    za2_next = wire.send(g_block(zn, every_row, cols_a), ra2p, z_next)
    b_first(1)
    b_second(0)
    pass_on(3)

    gradient(2)
    za1[1].wait_recv()
    view = g_block(zb, upper, cols_a)
    add3(view, view, ra1m)
    za2_back = wire.send(g_block(zb, every_row, cols_a), ra2m, z_back)
    b_first(2)
    b_second(1)
    b_sum(0)
    zb1 = (
        wire.send(s_block(zf, own_low), zb1p, z_next),
        wire.send(s_block(zf, own_high), zb1m, z_back),
    )

    gradient(3)
    b_first(3)
    za2_next.wait_recv()
    za2_back.wait_recv()
    add3(sum_a, g_block(z, every_row, cols_a), ra2p, ra2m)

    def a_block(rows):
        return sum_a.at[all_p, rows, :]

    ya1 = (
        wire.send(a_block(low_rows_of(yf)), ya1p, y_next),
        wire.send(a_block(high_rows_of(yf)), ya1m, y_back),
    )
    b_second(2)
    b_sum(1)
    zb1[0].wait_recv()
    view = s_block(zn, own_low)
    add3(view, view, zb1p)
    zb2_next = wire.send(sum_b.at[zn], zb2p, z_next)
    b_second(3)
    ya1[0].wait_recv()
    view = a_block(low_rows_of(yn))
    add3(view, view, ya1p)
    ya2_next = wire.send(a_block(rows_of(yn)), ya2p, y_next)
    ya1[1].wait_recv()
    view = a_block(high_rows_of(yb))
    add3(view, view, ya1m)
    ya2_back = wire.send(a_block(rows_of(yb)), ya2m, y_back)
    b_sum(2)
    zb1[1].wait_recv()
    view = s_block(zb, own_high)
    add3(view, view, zb1m)
    zb2_back = wire.send(sum_b.at[zb], zb2m, z_back)
    b_sum(3)
    ya2_next.wait_recv()
    ya2_back.wait_recv()
    add3(final.at[all_p, pl.ds(0, pair_rows), cols_a], a_block(rows_of(y)), ya2p, ya2m)
    zb2_next.wait_recv()
    zb2_back.wait_recv()
    add3(final.at[all_p, pl.ds(0, pair_rows), cols_b], sum_b.at[z], zb2p, zb2m)

    kept = pl.ds(pl.multiple_of(x_hi * own_rows, own_rows), own_rows)
    given = pl.ds(pl.multiple_of((1 - x_hi) * own_rows, own_rows), own_rows)
    last = wire.send(final.at[all_p, given, :], crossed, x_far)
    out_pair[:, :, x_hi_cols] = final[0:2, kept, :]
    out_down[:, x_hi_cols] = final[2, kept, :]
    last.wait_recv()
    out_pair[:, :, other_cols] = crossed[0:2]
    out_down[:, other_cols] = crossed[2]
    wire.drain()


def per_device(x_pool, token_ids, cotangent, gate_up, down_weight, loss_exponent):
    tokens, width = cotangent.shape
    quarter = width // 4
    half = quarter // 2
    own_rows = down_weight.shape[0]
    pair_rows, chunk_rows = 2 * own_rows, 8 * own_rows
    chip_tokens, ring_tokens = 2 * tokens, 8 * tokens
    acts = 3 * chunk_rows

    def held(*shape, dtype=BF16):
        return pltpu.VMEM(shape, dtype)

    scratch = [
        held(ring_tokens, quarter), held(ring_tokens, quarter),
        held(tokens, quarter), held(tokens, quarter),
        held(3, tokens, quarter), held(4, x_pool.shape[0], quarter),
        held(4, 3, chunk_rows, quarter),
        held(4, 4, chip_tokens, acts), held(4, chip_tokens, acts, dtype=F32),
        held(4, tokens, acts), held(4, tokens, acts),
        held(4, chip_tokens, acts), held(4, chip_tokens, acts),
        held(4, 3, chunk_rows, ring_tokens),
        held(4, 3, chunk_rows, quarter),
        held(3, chunk_rows // 2, half), held(3, chunk_rows // 2, half),
        held(3, chunk_rows, half), held(3, chunk_rows, half),
        held(3, chunk_rows, half),
        held(3, own_rows, half), held(3, own_rows, half),
        held(3, pair_rows, half), held(3, pair_rows, half),
        held(4, 3, own_rows, half), held(4, 3, own_rows, half),
        held(4, 3, pair_rows, half), held(4, 3, pair_rows, half),
        held(4, 3, pair_rows, half),
        held(3, own_rows, half), held(3, own_rows, half),
        held(3, pair_rows, half), held(3, pair_rows, half),
        held(3, pair_rows, quarter), held(3, own_rows, quarter),
        pltpu.SemaphoreType.DMA((COPIES,)),
        pltpu.SemaphoreType.DMA((COPIES,)),
        pltpu.SemaphoreType.DMA((LOCALS,)),
    ]
    far = pl.BlockSpec(memory_space=pl.ANY)
    near = pl.BlockSpec(memory_space=pltpu.VMEM)
    return pl.pallas_call(
        kernel,
        out_shape=(
            jax.ShapeDtypeStruct(gate_up.shape, BF16),
            jax.ShapeDtypeStruct(down_weight.shape, BF16),
        ),
        in_specs=[far, near, far, far, far, pl.BlockSpec(memory_space=pltpu.SMEM)],
        out_specs=(near, near),
        scratch_shapes=scratch,
        compiler_params=pltpu.CompilerParams(
            collective_id=0, has_side_effects=True, vmem_limit_bytes=64_000_000
        ),
    )(x_pool, token_ids.reshape(1, tokens), cotangent, gate_up, down_weight, loss_exponent)


def solution(mesh):
    in_specs = (
        P(("grp", "wide"), None),
        P(("grp", "wide")),
        P(("grp", "wide"), None),
        P(None, "wide", "grp"),
        P("wide", "grp"),
        P(),
    )
    out_specs = (P(None, "wide", "grp"), P("wide", "grp"))
    return jax.shard_map(
        per_device, mesh=mesh, in_specs=in_specs, out_specs=out_specs, check_vma=False
    )
```

```python
import functools

import jax
import jax.numpy as jnp
from jax import lax
from jax.experimental import pallas as pl
from jax.experimental.pallas import tpu as pltpu
from jax.sharding import PartitionSpec as P

MESH = pl.DeviceIdType.MESH
BF16 = jnp.bfloat16
F32 = jnp.float32
COPIES = 128
LOCALS = 16
TILE = 256


def dot_nt(a, b):
    return lax.dot_general(a, b, (((1,), (1,)), ((), ())), preferred_element_type=F32)


def dot_nn(a, b):
    return lax.dot_general(a, b, (((1,), (0,)), ((), ())), preferred_element_type=F32)


def split_columns(quarter):
    tiles = quarter // TILE
    low = max(1, 3 * tiles // 7)
    return low * TILE, (tiles - low) * TILE


class Wire:
    def __init__(self, send_sems, recv_sems):
        self.send_sems, self.recv_sems = send_sems, recv_sems
        self.count = 0
        self.sent = []

    def send(self, src, dst, device):
        copy = pltpu.make_async_remote_copy(
            src_ref=src,
            dst_ref=dst,
            send_sem=self.send_sems.at[self.count],
            recv_sem=self.recv_sems.at[self.count],
            device_id=device,
            device_id_type=MESH,
        )
        self.count += 1
        copy.start()
        self.sent.append(copy)
        return copy

    def drain(self):
        for copy in self.sent:
            copy.wait_send()


def kernel(
    pool, ids, cot, gate_up, down, exponent,
    out_pair, out_down,
    tok_x, tok_c, via_x, via_c, picked, pool_q, weights,
    part, part_own, r1p, r1m, r2p, r2m, deltas, grads,
    ring_a, sum_a, ya1p, ya1m, ya2p, ya2m,
    yb1p, yb1m, yb2p, yb2m, sum_b, ring_b,
    final, crossed, send_sems, recv_sems, local_sems,
):
    tokens, width = cot.shape
    quarter = width // 4
    half = quarter // 2
    own_rows = down.shape[0]
    pair_rows = 2 * own_rows
    chunk_rows = 4 * pair_rows
    chip_tokens = 2 * tokens
    pool_rows = pool.shape[0]
    tile = TILE
    part_a, part_b = split_columns(quarter)

    x_lo = lax.axis_index("grp")
    wide = lax.axis_index("wide")
    z = lax.div(wide, 16)
    x_hi = lax.rem(lax.div(wide, 8), 2)
    y = lax.rem(lax.div(wide, 2), 4)
    core = lax.rem(wide, 2)
    x = 2 * x_hi + x_lo
    device_index = x_lo * 64 + wide

    def shift(v, by):
        return lax.rem(v + (by % 4), 4)

    def device(xx, yy, zz, cc):
        return (lax.rem(xx, 2), zz * 16 + lax.div(xx, 2) * 8 + yy * 2 + cc)

    xn, xf, xb = shift(x, 1), shift(x, 2), shift(x, -1)
    yn, yf, yb = shift(y, 1), shift(y, 2), shift(y, -1)
    zn, zf, zb = shift(z, 1), shift(z, 2), shift(z, -1)
    z_on, z_off = (lax.rem(z + 4 + s, 4) for s in (1 - 2 * core, 2 * core - 1))
    x_next, x_far, x_back = (device(v, y, z, core) for v in (xn, xf, xb))
    y_next, y_back = (device(x, v, z, core) for v in (yn, yb))
    z_next, z_back = (device(x, y, v, core) for v in (zn, zb))
    z_ring = device(x, y, z_on, core)
    partner = device(x, y, z, 1 - core)

    def feature_quarter(xx):
        return 2 * lax.rem(xx, 2) + lax.div(xx, 2)

    def q_cols(xx):
        return pl.ds(pl.multiple_of(feature_quarter(xx) * quarter, quarter), quarter)

    def slot(xx, cc):
        return pl.ds(pl.multiple_of((2 * xx + cc) * tokens, tokens), tokens)

    def chip_slot(xx):
        return pl.ds(pl.multiple_of(xx * chip_tokens, chip_tokens), chip_tokens)

    def rows_of(yy):
        return pl.ds(pl.multiple_of(yy * pair_rows, pair_rows), pair_rows)

    def low_rows_of(yy):
        return pl.ds(pl.multiple_of(yy * pair_rows, own_rows), own_rows)

    def high_rows_of(yy):
        return pl.ds(pl.multiple_of(yy * pair_rows + own_rows, own_rows), own_rows)

    def owner_rows(xh):
        return pl.ds(pl.multiple_of(y * pair_rows + xh * own_rows, own_rows), own_rows)

    cols_a = pl.ds(0, half)
    cols_b = pl.ds(half, half)
    all_p = pl.ds(0, 3)
    wire = Wire(send_sems, recv_sems)
    locals_used = [0]

    def fetch(src, dst):
        copy = pltpu.make_async_copy(src, dst, local_sems.at[locals_used[0]])
        locals_used[0] += 1
        copy.start()
        return copy

    far_pool = fetch(pool.at[:, q_cols(xf)], pool_q.at[0])

    barrier = pltpu.get_barrier_semaphore()
    for peer in (x_next, x_back, x_far, y_next, y_back, z_next, z_back, partner):
        pl.semaphore_signal(barrier, inc=1, device_id=peer, device_id_type=MESH)
    pl.semaphore_wait(barrier, 8)

    x_hi_cols = pl.ds(pl.multiple_of(x_hi * quarter, quarter), quarter)
    other_cols = pl.ds(pl.multiple_of((1 - x_hi) * quarter, quarter), quarter)
    wx_pair = wire.send(
        gate_up.at[:, :, other_cols], weights.at[z, pl.ds(0, 2), owner_rows(x_hi), :], x_far
    )
    wx_down = wire.send(down.at[:, other_cols], weights.at[z, 2, owner_rows(x_hi), :], x_far)
    w_pair = fetch(gate_up.at[:, :, x_hi_cols], weights.at[z, pl.ds(0, 2), owner_rows(x_hi), :])
    w_down = fetch(down.at[:, x_hi_cols], weights.at[z, 2, owner_rows(x_hi), :])

    c_via = wire.send(cot.at[:, q_cols(xf)], via_c, x_back)
    c_back = wire.send(cot.at[:, q_cols(xb)], tok_c.at[slot(x, core), :], x_back)
    c_own = fetch(cot.at[:, q_cols(x)], tok_c.at[slot(x, core), :])
    next_pool = fetch(pool.at[:, q_cols(xn)], pool_q.at[1])
    back_pool = fetch(pool.at[:, q_cols(xb)], pool_q.at[2])
    own_pool = fetch(pool.at[:, q_cols(x)], pool_q.at[3])

    local_ids = ids[...] - device_index * pool_rows
    row_ids = lax.broadcasted_iota(jnp.int32, (pool_rows, tokens), 0)
    chosen = jnp.where(row_ids == local_ids, 1.0, 0.0).astype(F32).T.astype(BF16)

    def pick(index, target, row_slot):
        def step(n, carry):
            cols = pl.ds(pl.multiple_of(n * tile, tile), tile)
            target[row_slot, cols] = dot_nn(chosen, pool_q[index, :, cols]).astype(BF16)
            return carry

        lax.fori_loop(0, quarter // tile, step, 0)

    every = pl.ds(0, tokens)
    far_pool.wait()
    pick(0, picked.at[0], every)
    x_via = wire.send(picked.at[0], via_x, x_next)
    c_next = wire.send(cot.at[:, q_cols(xn)], tok_c.at[slot(x, core), :], x_next)

    w_pair.wait()
    w_down.wait()
    wx_pair.wait_recv()
    wx_down.wait_recv()

    def w_block(zz, rows, cols):
        return weights.at[zz, all_p, rows, cols]

    def same(view, device_):
        return wire.send(view, view, device_)

    a_next = same(w_block(z, rows_of(y), cols_a), y_next)
    a_back = same(w_block(z, rows_of(y), cols_a), y_back)
    b_next = same(w_block(z, rows_of(y), cols_b), z_next)
    b_back = same(w_block(z, rows_of(y), cols_b), z_back)

    own_pool.wait()
    pick(3, tok_x, slot(x, core))
    dd_own_x = same(tok_x.at[slot(x, core), :], partner)
    c_own.wait()
    dd_own_c = same(tok_c.at[slot(x, core), :], partner)
    next_pool.wait()
    pick(1, picked.at[1], every)
    back_pool.wait()
    pick(2, picked.at[2], every)

    a_next.wait_recv()
    a_on = same(w_block(z, low_rows_of(yb), cols_a), y_next)
    a_back.wait_recv()
    a_off = same(w_block(z, high_rows_of(yn), cols_a), y_back)
    b_next.wait_recv()
    b_on = same(w_block(zb, low_rows_of(y), cols_b), z_next)
    b_back.wait_recv()
    b_off = same(w_block(zn, high_rows_of(y), cols_b), z_back)

    a_on.wait_recv()
    a_off.wait_recv()
    every_row = pl.ds(0, chunk_rows)
    lower, upper = pl.ds(0, chunk_rows // 2), pl.ds(chunk_rows // 2, chunk_rows // 2)
    a2_next = same(w_block(z, every_row, cols_a), z_next)
    a2_back = same(w_block(z, every_row, cols_a), z_back)
    b_on.wait_recv()
    b_off.wait_recv()
    b2_next = same(w_block(pl.ds(0, 4), rows_of(y), cols_b), y_next)
    b2_back = same(w_block(pl.ds(0, 4), rows_of(y), cols_b), y_back)

    c_via.wait_recv()
    c_pass = wire.send(via_c, tok_c.at[slot(xn, core), :], x_back)
    x_back_copy = wire.send(picked.at[2], tok_x.at[slot(x, core), :], x_back)
    x_via.wait_recv()
    x_pass = wire.send(via_x, tok_x.at[slot(xb, core), :], x_next)
    x_next_copy = wire.send(picked.at[1], tok_x.at[slot(x, core), :], x_next)

    c_back.wait_recv()
    dd_c_n = same(tok_c.at[slot(xn, core), :], partner)
    c_next.wait_recv()
    dd_c_b = same(tok_c.at[slot(xb, core), :], partner)

    a2_next.wait_recv()
    a2_on = same(w_block(zb, lower, cols_a), z_next)
    a2_back.wait_recv()
    a2_off = same(w_block(zn, upper, cols_a), z_back)
    b2_next.wait_recv()
    b2_on = same(w_block(pl.ds(0, 2), rows_of(yb), cols_b), y_next)
    b2_back.wait_recv()
    b2_off = same(w_block(pl.ds(2, 2), rows_of(yn), cols_b), y_back)

    c_pass.wait_recv()
    dd_c_f = same(tok_c.at[slot(xf, core), :], partner)
    x_pass.wait_recv()
    dd_x_f = same(tok_x.at[slot(xf, core), :], partner)

    for copy in (a2_on, a2_off, b2_on, b2_off):
        copy.wait_recv()

    def forward(xx, target):
        def step(j, carry):
            tx = tok_x[chip_slot(xx), :]
            for h in range(2):
                pair = weights[2 * j + h, 0:2].reshape(2 * chunk_rows, quarter)
                target[2 * j + h, :, 0 : 2 * chunk_rows] = dot_nt(tx, pair).astype(target.dtype)
            tc = tok_c[chip_slot(xx), :]
            both = weights[pl.ds(2 * j, 2), 2].reshape(2 * chunk_rows, quarter)
            back = dot_nt(tc, both).astype(target.dtype)
            target[2 * j, :, 2 * chunk_rows :] = back[:, :chunk_rows]
            target[2 * j + 1, :, 2 * chunk_rows :] = back[:, chunk_rows:]
            return carry

        lax.fori_loop(0, 2, step, 0)

    first, second = pl.ds(0, tokens), pl.ds(tokens, tokens)
    dd_c_f.wait_recv()
    dd_x_f.wait_recv()
    forward(xf, part.at[xf])
    order = (z_off, zf, z_on, z)
    rs1 = []
    for zz in order:
        rs1.append(
            (
                wire.send(part.at[xf, zz, first, :], r1p.at[zz], x_next),
                wire.send(part.at[xf, zz, second, :], r1m.at[zz], x_back),
            )
        )
    dd_own_x.wait_recv()
    dd_own_c.wait_recv()
    forward(x, part_own)

    x_back_copy.wait_recv()
    dd_x_n = same(tok_x.at[slot(xn, core), :], partner)
    x_next_copy.wait_recv()
    dd_x_b = same(tok_x.at[slot(xb, core), :], partner)
    dd_c_n.wait_recv()
    dd_x_n.wait_recv()
    forward(xn, part.at[xn])
    dd_c_b.wait_recv()
    dd_x_b.wait_recv()
    forward(xb, part.at[xb])

    def add_into(ref, *others):
        total = ref[...].astype(F32)
        for other in others:
            total = total + other[...].astype(F32)
        ref[...] = total.astype(ref.dtype)

    def own_lanes(xx):
        return pl.ds(pl.multiple_of(xx * chip_tokens, chip_tokens), chip_tokens)

    def low_lanes(xx):
        return pl.ds(pl.multiple_of(xx * chip_tokens, tokens), tokens)

    def high_lanes(xx):
        return pl.ds(pl.multiple_of(xx * chip_tokens + tokens, tokens), tokens)

    level = exponent[0]
    unscale = jnp.float32(0.0)
    for power in range(16):
        unscale = jnp.where(level == power, jnp.float32(0.5**power), unscale)

    every_unit = pl.ds(0, chunk_rows)
    rs2, ag, passed, yb1, yb2 = {}, {}, {}, {}, {}

    def reduce_on(k):
        zz = order[k]
        rs1[k][0].wait_recv()
        add_into(part.at[xn, zz, first, :], r1p.at[zz])
        fwd = wire.send(part.at[xn, zz], r2p.at[zz], x_next)
        rs1[k][1].wait_recv()
        add_into(part.at[xb, zz, second, :], r1m.at[zz])
        rs2[k] = (fwd, wire.send(part.at[xb, zz], r2m.at[zz], x_back))

    def activate(k):
        zz = order[k]
        rs2[k][0].wait_recv()
        rs2[k][1].wait_recv()
        total = part_own[zz] + r2p[zz].astype(F32) + r2m[zz].astype(F32)
        gate = total[:, :chunk_rows]
        up = total[:, chunk_rows : 2 * chunk_rows]
        delta = unscale * total[:, 2 * chunk_rows :]
        sig = 1.0 / (1.0 + jnp.exp(-gate))
        hidden = gate * sig * up
        delta_gate = delta * up * sig * (1.0 + gate * (1.0 - sig))
        delta_up = delta * gate * sig
        deltas[zz, 0, :, own_lanes(x)] = delta_gate.T.astype(BF16)
        deltas[zz, 1, :, own_lanes(x)] = delta_up.T.astype(BF16)
        deltas[zz, 2, :, own_lanes(x)] = hidden.T.astype(BF16)

    def gather(k):
        mine = deltas.at[order[k], all_p, every_unit, own_lanes(x)]
        ag[k] = (same(mine, x_next), same(mine, x_back))

    def pass_on(k):
        zz = order[k]
        ag[k][0].wait_recv()
        on = same(deltas.at[zz, all_p, every_unit, low_lanes(xb)], x_next)
        ag[k][1].wait_recv()
        passed[k] = (on, same(deltas.at[zz, all_p, every_unit, high_lanes(xn)], x_back))

    def gathered(k):
        passed[k][0].wait_recv()
        passed[k][1].wait_recv()

    def grad_half(k, start, size):
        zz = order[k]

        def step(n, carry):
            cols = pl.ds(pl.multiple_of(start + n * tile, tile), tile)
            pair = deltas[zz, 0:2].reshape(2 * chunk_rows, 4 * chip_tokens)
            out = dot_nn(pair, tok_x[:, cols]).astype(BF16)
            grads[zz, 0, :, cols] = out[:chunk_rows]
            grads[zz, 1, :, cols] = out[chunk_rows:]
            down_part = unscale * dot_nn(deltas[zz, 2], tok_c[:, cols])
            grads[zz, 2, :, cols] = down_part.astype(BF16)
            return carry

        lax.fori_loop(0, size // tile, step, 0)

    cols_a, cols_b = pl.ds(0, part_a), pl.ds(part_a, part_b)

    def g_block(zz, rows, cols):
        return grads.at[zz, all_p, rows, cols]

    def add3(out, *terms):
        for p in range(3):
            total = terms[0][p].astype(F32)
            for term in terms[1:]:
                total = total + term[p].astype(F32)
            out[p] = total.astype(out.dtype)

    ring_of_a, ring_of_b = [], []

    def a_step(k):
        view = g_block(order[k], every_row, cols_a)
        if k > 0:
            ring_of_a[k - 1].wait_recv()
            add3(view, view, ring_a.at[k - 1])
        ring_of_a.append(wire.send(view, ring_a.at[k], z_ring))

    def b_step(k):
        view = sum_b.at[order[k]]
        if k > 0:
            ring_of_b[k - 1].wait_recv()
            add3(view, view, ring_b.at[k - 1])
        ring_of_b.append(wire.send(view, ring_b.at[k], z_ring))

    def b_first(k):
        zz = order[k]
        yb1[k] = (
            wire.send(g_block(zz, low_rows_of(yf), cols_b), yb1p.at[zz], y_next),
            wire.send(g_block(zz, high_rows_of(yf), cols_b), yb1m.at[zz], y_back),
        )

    def b_second(k):
        zz = order[k]
        yb1[k][0].wait_recv()
        view = g_block(zz, low_rows_of(yn), cols_b)
        add3(view, view, yb1p.at[zz])
        on = wire.send(g_block(zz, rows_of(yn), cols_b), yb2p.at[zz], y_next)
        yb1[k][1].wait_recv()
        view = g_block(zz, high_rows_of(yb), cols_b)
        add3(view, view, yb1m.at[zz])
        yb2[k] = (on, wire.send(g_block(zz, rows_of(yb), cols_b), yb2m.at[zz], y_back))

    def b_sum(k):
        zz = order[k]
        yb2[k][0].wait_recv()
        yb2[k][1].wait_recv()
        add3(sum_b.at[zz], g_block(zz, rows_of(y), cols_b), yb2p.at[zz], yb2m.at[zz])

    reduce_on(0)
    reduce_on(1)
    activate(0)
    gather(0)
    reduce_on(2)
    activate(1)
    pass_on(0)
    gather(1)
    reduce_on(3)
    activate(2)

    gathered(0)
    grad_half(0, 0, part_a)
    a_step(0)
    grad_half(0, part_a, part_b)
    b_first(0)
    pass_on(1)
    gather(2)
    b_second(0)
    activate(3)
    gather(3)

    gathered(1)
    grad_half(1, 0, part_a)
    a_step(1)
    grad_half(1, part_a, part_b)
    b_first(1)
    pass_on(2)
    b_sum(0)
    b_step(0)
    b_second(1)
    pass_on(3)

    gathered(2)
    grad_half(2, 0, part_a)
    a_step(2)
    grad_half(2, part_a, part_b)
    b_first(2)
    b_sum(1)
    b_step(1)

    gathered(3)
    grad_half(3, part_a, part_b)
    b_first(3)
    b_second(2)
    grad_half(3, 0, part_a)
    b_second(3)
    ring_of_a[2].wait_recv()
    add3(sum_a, g_block(z, every_row, cols_a), ring_a.at[2])

    def a_block(rows):
        return sum_a.at[all_p, rows, :]

    ya1 = (
        wire.send(a_block(low_rows_of(yf)), ya1p, y_next),
        wire.send(a_block(high_rows_of(yf)), ya1m, y_back),
    )
    b_sum(2)
    b_step(2)
    ya1[0].wait_recv()
    view = a_block(low_rows_of(yn))
    add3(view, view, ya1p)
    ya2_next = wire.send(a_block(rows_of(yn)), ya2p, y_next)
    ya1[1].wait_recv()
    view = a_block(high_rows_of(yb))
    add3(view, view, ya1m)
    ya2_back = wire.send(a_block(rows_of(yb)), ya2m, y_back)
    b_sum(3)
    ring_of_b[2].wait_recv()
    every_pair = pl.ds(0, pair_rows)
    add3(final.at[all_p, every_pair, cols_b], sum_b.at[z], ring_b.at[2])
    kept = pl.ds(pl.multiple_of(x_hi * own_rows, own_rows), own_rows)
    given = pl.ds(pl.multiple_of((1 - x_hi) * own_rows, own_rows), own_rows)
    every_own = pl.ds(0, own_rows)
    last_b = wire.send(
        final.at[all_p, given, cols_b], crossed.at[all_p, every_own, cols_b], x_far
    )
    ya2_next.wait_recv()
    ya2_back.wait_recv()
    add3(final.at[all_p, every_pair, cols_a], a_block(rows_of(y)), ya2p, ya2m)
    last_a = wire.send(
        final.at[all_p, given, cols_a], crossed.at[all_p, every_own, cols_a], x_far
    )
    out_pair[:, :, x_hi_cols] = final[0:2, kept, :]
    out_down[:, x_hi_cols] = final[2, kept, :]
    last_b.wait_recv()
    last_a.wait_recv()
    out_pair[:, :, other_cols] = crossed[0:2]
    out_down[:, other_cols] = crossed[2]
    wire.drain()


def per_device(x_pool, token_ids, cotangent, gate_up, down_weight, loss_exponent):
    tokens, width = cotangent.shape
    quarter = width // 4
    half = quarter // 2
    own_rows = down_weight.shape[0]
    pair_rows, chunk_rows = 2 * own_rows, 8 * own_rows
    chip_tokens, ring_tokens = 2 * tokens, 8 * tokens
    acts = 3 * chunk_rows
    part_a, part_b = split_columns(quarter)

    def held(*shape, dtype=BF16):
        return pltpu.VMEM(shape, dtype)

    scratch = [
        held(ring_tokens, quarter), held(ring_tokens, quarter),
        held(tokens, quarter), held(tokens, quarter),
        held(3, tokens, quarter), held(4, x_pool.shape[0], quarter),
        held(4, 3, chunk_rows, quarter),
        held(4, 4, chip_tokens, acts), held(4, chip_tokens, acts, dtype=F32),
        held(4, tokens, acts), held(4, tokens, acts),
        held(4, chip_tokens, acts), held(4, chip_tokens, acts),
        held(4, 3, chunk_rows, ring_tokens),
        held(4, 3, chunk_rows, quarter),
        held(3, 3, chunk_rows, part_a), held(3, chunk_rows, part_a),
        held(3, own_rows, part_a), held(3, own_rows, part_a),
        held(3, pair_rows, part_a), held(3, pair_rows, part_a),
        held(4, 3, own_rows, part_b), held(4, 3, own_rows, part_b),
        held(4, 3, pair_rows, part_b), held(4, 3, pair_rows, part_b),
        held(4, 3, pair_rows, part_b), held(3, 3, pair_rows, part_b),
        held(3, pair_rows, quarter), held(3, own_rows, quarter),
        pltpu.SemaphoreType.DMA((COPIES,)),
        pltpu.SemaphoreType.DMA((COPIES,)),
        pltpu.SemaphoreType.DMA((LOCALS,)),
    ]
    far = pl.BlockSpec(memory_space=pl.ANY)
    near = pl.BlockSpec(memory_space=pltpu.VMEM)
    return pl.pallas_call(
        kernel,
        out_shape=(
            jax.ShapeDtypeStruct(gate_up.shape, BF16),
            jax.ShapeDtypeStruct(down_weight.shape, BF16),
        ),
        in_specs=[far, near, far, far, far, pl.BlockSpec(memory_space=pltpu.SMEM)],
        out_specs=(near, near),
        scratch_shapes=scratch,
        compiler_params=pltpu.CompilerParams(
            collective_id=0, has_side_effects=True, vmem_limit_bytes=64_000_000
        ),
    )(x_pool, token_ids.reshape(1, tokens), cotangent, gate_up, down_weight, loss_exponent)


def solution(mesh):
    in_specs = (
        P(("grp", "wide"), None),
        P(("grp", "wide")),
        P(("grp", "wide"), None),
        P(None, "wide", "grp"),
        P("wide", "grp"),
        P(),
    )
    out_specs = (P(None, "wide", "grp"), P("wide", "grp"))
    return jax.shard_map(
        per_device, mesh=mesh, in_specs=in_specs, out_specs=out_specs, check_vma=False
    )
```

```python
import functools

import jax
import jax.numpy as jnp
from jax import lax
from jax.experimental import pallas as pl
from jax.experimental.pallas import tpu as pltpu
from jax.sharding import PartitionSpec as P

MESH = pl.DeviceIdType.MESH
BF16 = jnp.bfloat16
F32 = jnp.float32
COPIES = 128
LOCALS = 16
TILE = 256


def dot_nt(a, b):
    return lax.dot_general(a, b, (((1,), (1,)), ((), ())), preferred_element_type=F32)


def dot_nn(a, b):
    return lax.dot_general(a, b, (((1,), (0,)), ((), ())), preferred_element_type=F32)


def split_columns(quarter):
    tiles = quarter // TILE
    low = max(1, 3 * tiles // 7)
    return low * TILE, (tiles - low) * TILE


class Wire:
    def __init__(self, send_sems, recv_sems):
        self.send_sems, self.recv_sems = send_sems, recv_sems
        self.count = 0
        self.sent = []

    def send(self, src, dst, device):
        copy = pltpu.make_async_remote_copy(
            src_ref=src,
            dst_ref=dst,
            send_sem=self.send_sems.at[self.count],
            recv_sem=self.recv_sems.at[self.count],
            device_id=device,
            device_id_type=MESH,
        )
        self.count += 1
        copy.start()
        self.sent.append(copy)
        return copy

    def drain(self):
        for copy in self.sent:
            copy.wait_send()


def kernel(
    pool, ids, cot, gate_up, down, exponent,
    out_pair, out_down,
    tok_x, tok_c, via_x, via_c, picked, pool_q, weights,
    part, part_own, r1p, r1m, r2p, r2m, deltas, grads,
    ring_a, sum_a, ya1p, ya1m, ya2p, ya2m,
    yb1p, yb1m, yb2p, yb2m, sum_b, ring_b,
    final, crossed, ids_v, send_sems, recv_sems, local_sems,
):
    tokens, width = cot.shape
    quarter = width // 4
    half = quarter // 2
    own_rows = down.shape[0]
    pair_rows = 2 * own_rows
    chunk_rows = 4 * pair_rows
    chip_tokens = 2 * tokens
    pool_rows = pool.shape[0]
    tile = TILE
    part_a, part_b = split_columns(quarter)

    x_lo = lax.axis_index("grp")
    wide = lax.axis_index("wide")
    z = lax.div(wide, 16)
    x_hi = lax.rem(lax.div(wide, 8), 2)
    y = lax.rem(lax.div(wide, 2), 4)
    core = lax.rem(wide, 2)
    x = 2 * x_hi + x_lo
    device_index = x_lo * 64 + wide

    def shift(v, by):
        return lax.rem(v + (by % 4), 4)

    def device(xx, yy, zz, cc):
        return (lax.rem(xx, 2), zz * 16 + lax.div(xx, 2) * 8 + yy * 2 + cc)

    xn, xf, xb = shift(x, 1), shift(x, 2), shift(x, -1)
    yn, yf, yb = shift(y, 1), shift(y, 2), shift(y, -1)
    zn, zf, zb = shift(z, 1), shift(z, 2), shift(z, -1)
    z_on, z_off = (lax.rem(z + 4 + s, 4) for s in (1 - 2 * core, 2 * core - 1))
    x_next, x_far, x_back = (device(v, y, z, core) for v in (xn, xf, xb))
    y_next, y_back = (device(x, v, z, core) for v in (yn, yb))
    z_next, z_back = (device(x, y, v, core) for v in (zn, zb))
    z_ring = device(x, y, z_on, core)
    partner = device(x, y, z, 1 - core)

    def feature_quarter(xx):
        return 2 * lax.rem(xx, 2) + lax.div(xx, 2)

    def q_cols(xx):
        return pl.ds(pl.multiple_of(feature_quarter(xx) * quarter, quarter), quarter)

    def slot(xx, cc):
        return pl.ds(pl.multiple_of((2 * xx + cc) * tokens, tokens), tokens)

    def chip_slot(xx):
        return pl.ds(pl.multiple_of(xx * chip_tokens, chip_tokens), chip_tokens)

    def rows_of(yy):
        return pl.ds(pl.multiple_of(yy * pair_rows, pair_rows), pair_rows)

    def low_rows_of(yy):
        return pl.ds(pl.multiple_of(yy * pair_rows, own_rows), own_rows)

    def high_rows_of(yy):
        return pl.ds(pl.multiple_of(yy * pair_rows + own_rows, own_rows), own_rows)

    def owner_rows(xh):
        return pl.ds(pl.multiple_of(y * pair_rows + xh * own_rows, own_rows), own_rows)

    cols_a = pl.ds(0, half)
    cols_b = pl.ds(half, half)
    all_p = pl.ds(0, 3)
    wire = Wire(send_sems, recv_sems)
    locals_used = [0]

    def fetch(src, dst):
        copy = pltpu.make_async_copy(src, dst, local_sems.at[locals_used[0]])
        locals_used[0] += 1
        copy.start()
        return copy

    ids_here = fetch(ids, ids_v)
    far_pool = fetch(pool.at[:, q_cols(xf)], pool_q.at[0])

    barrier = pltpu.get_barrier_semaphore()
    for peer in (x_next, x_back, x_far, y_next, y_back, z_next, z_back, partner):
        pl.semaphore_signal(barrier, inc=1, device_id=peer, device_id_type=MESH)
    pl.semaphore_wait(barrier, 8)

    x_hi_cols = pl.ds(pl.multiple_of(x_hi * quarter, quarter), quarter)
    other_cols = pl.ds(pl.multiple_of((1 - x_hi) * quarter, quarter), quarter)
    wx_pair = wire.send(
        gate_up.at[:, :, other_cols], weights.at[z, pl.ds(0, 2), owner_rows(x_hi), :], x_far
    )
    wx_down = wire.send(down.at[:, other_cols], weights.at[z, 2, owner_rows(x_hi), :], x_far)
    w_pair = fetch(gate_up.at[:, :, x_hi_cols], weights.at[z, pl.ds(0, 2), owner_rows(x_hi), :])
    w_down = fetch(down.at[:, x_hi_cols], weights.at[z, 2, owner_rows(x_hi), :])

    c_via = wire.send(cot.at[:, q_cols(xf)], via_c, x_back)
    c_back = wire.send(cot.at[:, q_cols(xb)], tok_c.at[slot(x, core), :], x_back)
    c_own = fetch(cot.at[:, q_cols(x)], tok_c.at[slot(x, core), :])
    next_pool = fetch(pool.at[:, q_cols(xn)], pool_q.at[1])
    back_pool = fetch(pool.at[:, q_cols(xb)], pool_q.at[2])
    own_pool = fetch(pool.at[:, q_cols(x)], pool_q.at[3])

    ids_here.wait()
    local_ids = ids_v[...] - device_index * pool_rows
    row_ids = lax.broadcasted_iota(jnp.int32, (pool_rows, tokens), 0)
    chosen = jnp.where(row_ids == local_ids, 1.0, 0.0).astype(F32).T.astype(BF16)

    def pick(index, target, row_slot):
        def step(n, carry):
            cols = pl.ds(pl.multiple_of(n * tile, tile), tile)
            target[row_slot, cols] = dot_nn(chosen, pool_q[index, :, cols]).astype(BF16)
            return carry

        lax.fori_loop(0, quarter // tile, step, 0)

    every = pl.ds(0, tokens)
    far_pool.wait()
    pick(0, picked.at[0], every)
    x_via = wire.send(picked.at[0], via_x, x_next)
    c_next = wire.send(cot.at[:, q_cols(xn)], tok_c.at[slot(x, core), :], x_next)

    w_pair.wait()
    w_down.wait()
    wx_pair.wait_recv()
    wx_down.wait_recv()

    def w_block(zz, rows, cols):
        return weights.at[zz, all_p, rows, cols]

    def same(view, device_):
        return wire.send(view, view, device_)

    a_next = same(w_block(z, rows_of(y), cols_a), y_next)
    a_back = same(w_block(z, rows_of(y), cols_a), y_back)
    b_next = same(w_block(z, rows_of(y), cols_b), z_next)
    b_back = same(w_block(z, rows_of(y), cols_b), z_back)

    own_pool.wait()
    pick(3, tok_x, slot(x, core))
    dd_own_x = same(tok_x.at[slot(x, core), :], partner)
    c_own.wait()
    dd_own_c = same(tok_c.at[slot(x, core), :], partner)
    next_pool.wait()
    pick(1, picked.at[1], every)
    back_pool.wait()
    pick(2, picked.at[2], every)

    a_next.wait_recv()
    a_on = same(w_block(z, low_rows_of(yb), cols_a), y_next)
    a_back.wait_recv()
    a_off = same(w_block(z, high_rows_of(yn), cols_a), y_back)
    b_next.wait_recv()
    b_on = same(w_block(zb, low_rows_of(y), cols_b), z_next)
    b_back.wait_recv()
    b_off = same(w_block(zn, high_rows_of(y), cols_b), z_back)

    a_on.wait_recv()
    a_off.wait_recv()
    every_row = pl.ds(0, chunk_rows)
    lower, upper = pl.ds(0, chunk_rows // 2), pl.ds(chunk_rows // 2, chunk_rows // 2)
    a2_next = same(w_block(z, every_row, cols_a), z_next)
    a2_back = same(w_block(z, every_row, cols_a), z_back)
    b_on.wait_recv()
    b_off.wait_recv()
    b2_next = same(w_block(pl.ds(0, 4), rows_of(y), cols_b), y_next)
    b2_back = same(w_block(pl.ds(0, 4), rows_of(y), cols_b), y_back)

    c_via.wait_recv()
    c_pass = wire.send(via_c, tok_c.at[slot(xn, core), :], x_back)
    x_back_copy = wire.send(picked.at[2], tok_x.at[slot(x, core), :], x_back)
    x_via.wait_recv()
    x_pass = wire.send(via_x, tok_x.at[slot(xb, core), :], x_next)
    x_next_copy = wire.send(picked.at[1], tok_x.at[slot(x, core), :], x_next)

    c_back.wait_recv()
    dd_c_n = same(tok_c.at[slot(xn, core), :], partner)
    c_next.wait_recv()
    dd_c_b = same(tok_c.at[slot(xb, core), :], partner)

    a2_next.wait_recv()
    a2_on = same(w_block(zb, lower, cols_a), z_next)
    a2_back.wait_recv()
    a2_off = same(w_block(zn, upper, cols_a), z_back)
    b2_next.wait_recv()
    b2_on = same(w_block(pl.ds(0, 2), rows_of(yb), cols_b), y_next)
    b2_back.wait_recv()
    b2_off = same(w_block(pl.ds(2, 2), rows_of(yn), cols_b), y_back)

    c_pass.wait_recv()
    dd_c_f = same(tok_c.at[slot(xf, core), :], partner)
    x_pass.wait_recv()
    dd_x_f = same(tok_x.at[slot(xf, core), :], partner)

    for copy in (a2_on, a2_off, b2_on, b2_off):
        copy.wait_recv()

    def forward(xx, target):
        def step(j, carry):
            tx = tok_x[chip_slot(xx), :]
            for h in range(2):
                pair = weights[2 * j + h, 0:2].reshape(2 * chunk_rows, quarter)
                target[2 * j + h, :, 0 : 2 * chunk_rows] = dot_nt(tx, pair).astype(target.dtype)
            tc = tok_c[chip_slot(xx), :]
            both = weights[pl.ds(2 * j, 2), 2].reshape(2 * chunk_rows, quarter)
            back = dot_nt(tc, both).astype(target.dtype)
            target[2 * j, :, 2 * chunk_rows :] = back[:, :chunk_rows]
            target[2 * j + 1, :, 2 * chunk_rows :] = back[:, chunk_rows:]
            return carry

        lax.fori_loop(0, 2, step, 0)

    first, second = pl.ds(0, tokens), pl.ds(tokens, tokens)
    dd_c_f.wait_recv()
    dd_x_f.wait_recv()
    forward(xf, part.at[xf])
    order = (z_off, zf, z_on, z)
    rs1 = []
    for zz in order:
        rs1.append(
            (
                wire.send(part.at[xf, zz, first, :], r1p.at[zz], x_next),
                wire.send(part.at[xf, zz, second, :], r1m.at[zz], x_back),
            )
        )
    dd_own_x.wait_recv()
    dd_own_c.wait_recv()
    forward(x, part_own)

    x_back_copy.wait_recv()
    dd_x_n = same(tok_x.at[slot(xn, core), :], partner)
    x_next_copy.wait_recv()
    dd_x_b = same(tok_x.at[slot(xb, core), :], partner)
    dd_c_n.wait_recv()
    dd_x_n.wait_recv()
    forward(xn, part.at[xn])
    dd_c_b.wait_recv()
    dd_x_b.wait_recv()
    forward(xb, part.at[xb])

    def add_into(ref, *others):
        total = ref[...].astype(F32)
        for other in others:
            total = total + other[...].astype(F32)
        ref[...] = total.astype(ref.dtype)

    def own_lanes(xx):
        return pl.ds(pl.multiple_of(xx * chip_tokens, chip_tokens), chip_tokens)

    def low_lanes(xx):
        return pl.ds(pl.multiple_of(xx * chip_tokens, tokens), tokens)

    def high_lanes(xx):
        return pl.ds(pl.multiple_of(xx * chip_tokens + tokens, tokens), tokens)

    level = exponent[0]
    unscale = jnp.float32(0.0)
    for power in range(16):
        unscale = jnp.where(level == power, jnp.float32(0.5**power), unscale)

    every_unit = pl.ds(0, chunk_rows)
    rs2, ag, passed, yb1, yb2 = {}, {}, {}, {}, {}

    def reduce_on(k):
        zz = order[k]
        rs1[k][0].wait_recv()
        add_into(part.at[xn, zz, first, :], r1p.at[zz])
        fwd = wire.send(part.at[xn, zz], r2p.at[zz], x_next)
        rs1[k][1].wait_recv()
        add_into(part.at[xb, zz, second, :], r1m.at[zz])
        rs2[k] = (fwd, wire.send(part.at[xb, zz], r2m.at[zz], x_back))

    def activate(k):
        zz = order[k]
        rs2[k][0].wait_recv()
        rs2[k][1].wait_recv()
        total = part_own[zz] + r2p[zz].astype(F32) + r2m[zz].astype(F32)
        gate = total[:, :chunk_rows]
        up = total[:, chunk_rows : 2 * chunk_rows]
        delta = unscale * total[:, 2 * chunk_rows :]
        sig = 1.0 / (1.0 + jnp.exp(-gate))
        hidden = gate * sig * up
        delta_gate = delta * up * sig * (1.0 + gate * (1.0 - sig))
        delta_up = delta * gate * sig
        deltas[zz, 0, :, own_lanes(x)] = delta_gate.T.astype(BF16)
        deltas[zz, 1, :, own_lanes(x)] = delta_up.T.astype(BF16)
        deltas[zz, 2, :, own_lanes(x)] = hidden.T.astype(BF16)

    def gather(k):
        zz = order[k]
        low = deltas.at[zz, all_p, every_unit, low_lanes(x)]
        high = deltas.at[zz, all_p, every_unit, high_lanes(x)]
        early = (same(low, x_next), same(high, x_back))
        ag[k] = (early, (same(high, x_next), same(low, x_back)))

    def pass_on(k):
        zz = order[k]
        ag[k][0][0].wait_recv()
        on = same(deltas.at[zz, all_p, every_unit, low_lanes(xb)], x_next)
        ag[k][0][1].wait_recv()
        passed[k] = (on, same(deltas.at[zz, all_p, every_unit, high_lanes(xn)], x_back))

    def gathered(k):
        ag[k][1][0].wait_recv()
        ag[k][1][1].wait_recv()
        passed[k][0].wait_recv()
        passed[k][1].wait_recv()

    def grad_half(k, start, size):
        zz = order[k]

        def step(n, carry):
            cols = pl.ds(pl.multiple_of(start + n * tile, tile), tile)
            pair = deltas[zz, 0:2].reshape(2 * chunk_rows, 4 * chip_tokens)
            out = dot_nn(pair, tok_x[:, cols]).astype(BF16)
            grads[zz, 0, :, cols] = out[:chunk_rows]
            grads[zz, 1, :, cols] = out[chunk_rows:]
            down_part = unscale * dot_nn(deltas[zz, 2], tok_c[:, cols])
            grads[zz, 2, :, cols] = down_part.astype(BF16)
            return carry

        lax.fori_loop(0, size // tile, step, 0)

    cols_a, cols_b = pl.ds(0, part_a), pl.ds(part_a, part_b)

    def g_block(zz, rows, cols):
        return grads.at[zz, all_p, rows, cols]

    def add3(out, *terms):
        for p in range(3):
            total = terms[0][p].astype(F32)
            for term in terms[1:]:
                total = total + term[p].astype(F32)
            out[p] = total.astype(out.dtype)

    ring_of_a, ring_of_b = [], []

    def a_step(k):
        view = g_block(order[k], every_row, cols_a)
        if k > 0:
            ring_of_a[k - 1].wait_recv()
            add3(view, view, ring_a.at[k - 1])
        ring_of_a.append(wire.send(view, ring_a.at[k], z_ring))

    def b_step(k):
        view = sum_b.at[order[k]]
        if k > 0:
            ring_of_b[k - 1].wait_recv()
            add3(view, view, ring_b.at[k - 1])
        ring_of_b.append(wire.send(view, ring_b.at[k], z_ring))

    def b_first(k):
        zz = order[k]
        yb1[k] = (
            wire.send(g_block(zz, low_rows_of(yf), cols_b), yb1p.at[zz], y_next),
            wire.send(g_block(zz, high_rows_of(yf), cols_b), yb1m.at[zz], y_back),
        )

    def b_second(k):
        zz = order[k]
        yb1[k][0].wait_recv()
        view = g_block(zz, low_rows_of(yn), cols_b)
        add3(view, view, yb1p.at[zz])
        on = wire.send(g_block(zz, rows_of(yn), cols_b), yb2p.at[zz], y_next)
        yb1[k][1].wait_recv()
        view = g_block(zz, high_rows_of(yb), cols_b)
        add3(view, view, yb1m.at[zz])
        yb2[k] = (on, wire.send(g_block(zz, rows_of(yb), cols_b), yb2m.at[zz], y_back))

    def b_sum(k):
        zz = order[k]
        yb2[k][0].wait_recv()
        yb2[k][1].wait_recv()
        add3(sum_b.at[zz], g_block(zz, rows_of(y), cols_b), yb2p.at[zz], yb2m.at[zz])

    reduce_on(0)
    reduce_on(1)
    activate(0)
    gather(0)
    reduce_on(2)
    activate(1)
    pass_on(0)
    gather(1)
    reduce_on(3)
    activate(2)

    gathered(0)
    grad_half(0, 0, part_a)
    a_step(0)
    pass_on(1)
    gather(2)
    grad_half(0, part_a, part_b)
    b_first(0)
    b_second(0)
    activate(3)

    gathered(1)
    grad_half(1, 0, part_a)
    a_step(1)
    pass_on(2)
    gather(3)
    grad_half(1, part_a, part_b)
    b_first(1)
    b_sum(0)
    b_step(0)

    gathered(2)
    grad_half(2, 0, part_a)
    b_second(1)
    pass_on(3)
    grad_half(2, part_a, part_b)
    b_first(2)
    a_step(2)

    gathered(3)
    grad_half(3, part_a, part_b)
    b_first(3)
    b_second(2)
    b_sum(1)
    b_step(1)
    grad_half(3, 0, part_a)
    ring_of_a[2].wait_recv()
    add3(sum_a, g_block(z, every_row, cols_a), ring_a.at[2])

    def a_block(rows):
        return sum_a.at[all_p, rows, :]

    ya1 = (
        wire.send(a_block(low_rows_of(yf)), ya1p, y_next),
        wire.send(a_block(high_rows_of(yf)), ya1m, y_back),
    )
    b_second(3)
    b_sum(2)
    b_step(2)
    ya1[0].wait_recv()
    view = a_block(low_rows_of(yn))
    add3(view, view, ya1p)
    ya2_next = wire.send(a_block(rows_of(yn)), ya2p, y_next)
    ya1[1].wait_recv()
    view = a_block(high_rows_of(yb))
    add3(view, view, ya1m)
    ya2_back = wire.send(a_block(rows_of(yb)), ya2m, y_back)
    b_sum(3)
    ring_of_b[2].wait_recv()
    every_pair = pl.ds(0, pair_rows)
    add3(final.at[all_p, every_pair, cols_b], sum_b.at[z], ring_b.at[2])
    kept = pl.ds(pl.multiple_of(x_hi * own_rows, own_rows), own_rows)
    given = pl.ds(pl.multiple_of((1 - x_hi) * own_rows, own_rows), own_rows)
    every_own = pl.ds(0, own_rows)
    last_b = wire.send(
        final.at[all_p, given, cols_b], crossed.at[all_p, every_own, cols_b], x_far
    )
    ya2_next.wait_recv()
    ya2_back.wait_recv()
    add3(final.at[all_p, every_pair, cols_a], a_block(rows_of(y)), ya2p, ya2m)
    last_a = wire.send(
        final.at[all_p, given, cols_a], crossed.at[all_p, every_own, cols_a], x_far
    )
    out_pair[:, :, x_hi_cols] = final[0:2, kept, :]
    out_down[:, x_hi_cols] = final[2, kept, :]
    last_b.wait_recv()
    last_a.wait_recv()
    out_pair[:, :, other_cols] = crossed[0:2]
    out_down[:, other_cols] = crossed[2]
    wire.drain()


def per_device(x_pool, token_ids, cotangent, gate_up, down_weight, loss_exponent):
    tokens, width = cotangent.shape
    quarter = width // 4
    half = quarter // 2
    own_rows = down_weight.shape[0]
    pair_rows, chunk_rows = 2 * own_rows, 8 * own_rows
    chip_tokens, ring_tokens = 2 * tokens, 8 * tokens
    acts = 3 * chunk_rows
    part_a, part_b = split_columns(quarter)

    def held(*shape, dtype=BF16):
        return pltpu.VMEM(shape, dtype)

    scratch = [
        held(ring_tokens, quarter), held(ring_tokens, quarter),
        held(tokens, quarter), held(tokens, quarter),
        held(3, tokens, quarter), held(4, x_pool.shape[0], quarter),
        held(4, 3, chunk_rows, quarter),
        held(4, 4, chip_tokens, acts), held(4, chip_tokens, acts, dtype=F32),
        held(4, tokens, acts), held(4, tokens, acts),
        held(4, chip_tokens, acts), held(4, chip_tokens, acts),
        held(4, 3, chunk_rows, ring_tokens),
        held(4, 3, chunk_rows, quarter),
        held(3, 3, chunk_rows, part_a), held(3, chunk_rows, part_a),
        held(3, own_rows, part_a), held(3, own_rows, part_a),
        held(3, pair_rows, part_a), held(3, pair_rows, part_a),
        held(4, 3, own_rows, part_b), held(4, 3, own_rows, part_b),
        held(4, 3, pair_rows, part_b), held(4, 3, pair_rows, part_b),
        held(4, 3, pair_rows, part_b), held(3, 3, pair_rows, part_b),
        held(3, pair_rows, quarter), held(3, own_rows, quarter),
        pltpu.VMEM((1, tokens), jnp.int32),
        pltpu.SemaphoreType.DMA((COPIES,)),
        pltpu.SemaphoreType.DMA((COPIES,)),
        pltpu.SemaphoreType.DMA((LOCALS,)),
    ]
    far = pl.BlockSpec(memory_space=pltpu.HBM)
    near = pl.BlockSpec(memory_space=pltpu.VMEM)
    return pl.pallas_call(
        kernel,
        out_shape=(
            jax.ShapeDtypeStruct(gate_up.shape, BF16),
            jax.ShapeDtypeStruct(down_weight.shape, BF16),
        ),
        in_specs=[far, far, far, far, far, pl.BlockSpec(memory_space=pltpu.SMEM)],
        out_specs=(near, near),
        scratch_shapes=scratch,
        compiler_params=pltpu.CompilerParams(
            collective_id=0, has_side_effects=True, vmem_limit_bytes=56_000_000
        ),
    )(x_pool, token_ids.reshape(1, tokens), cotangent, gate_up, down_weight, loss_exponent)


def solution(mesh):
    in_specs = (
        P(("grp", "wide"), None),
        P(("grp", "wide")),
        P(("grp", "wide"), None),
        P(None, "wide", "grp"),
        P("wide", "grp"),
        P(),
    )
    out_specs = (P(None, "wide", "grp"), P("wide", "grp"))
    return jax.shard_map(
        per_device, mesh=mesh, in_specs=in_specs, out_specs=out_specs, check_vma=False
    )
```

```python
import functools

import jax
import jax.numpy as jnp
from jax import lax
from jax.experimental import pallas as pl
from jax.experimental.pallas import tpu as pltpu
from jax.sharding import PartitionSpec as P

MESH = pl.DeviceIdType.MESH
BF16 = jnp.bfloat16
F32 = jnp.float32
COPIES = 103
SENDS = 24
LOCALS = 8
TILE = 256


def dot_nt(a, b):
    return lax.dot_general(a, b, (((1,), (1,)), ((), ())), preferred_element_type=F32)


def dot_nn(a, b):
    return lax.dot_general(a, b, (((1,), (0,)), ((), ())), preferred_element_type=F32)


def split_columns(quarter):
    tiles = quarter // TILE
    low = max(1, 3 * tiles // 7)
    return low * TILE, (tiles - low) * TILE


class Wire:
    def __init__(self, send_sems, recv_sems):
        self.send_sems, self.recv_sems = send_sems, recv_sems
        self.count = 0
        self.sent = []

    def send(self, src, dst, device):
        lane = self.count % SENDS
        if self.count >= SENDS:
            self.sent[self.count - SENDS].wait_send()
        copy = pltpu.make_async_remote_copy(
            src_ref=src,
            dst_ref=dst,
            send_sem=self.send_sems.at[lane],
            recv_sem=self.recv_sems.at[self.count],
            device_id=device,
            device_id_type=MESH,
        )
        self.count += 1
        copy.start()
        self.sent.append(copy)
        return copy

    def drain(self):
        for copy in self.sent[-SENDS:]:
            copy.wait_send()


def kernel(
    pool, ids, cot, gate_up, down, exponent,
    out_pair, out_down,
    tok_x, tok_c, via_x, via_c, picked, pool_q, weights,
    part, part_own, r1p, r1m, r2p, r2m, deltas, grads,
    ring_a, sum_a, ya1p, ya1m, ya2p, ya2m,
    yb1p, yb1m, yb2p, yb2m, sum_b, ring_b,
    final, crossed, ids_v, send_sems, recv_sems, local_sems,
):
    tokens, width = cot.shape
    quarter = width // 4
    half = quarter // 2
    own_rows = down.shape[0]
    pair_rows = 2 * own_rows
    chunk_rows = 4 * pair_rows
    chip_tokens = 2 * tokens
    pool_rows = pool.shape[0]
    tile = TILE
    part_a, part_b = split_columns(quarter)

    x_lo = lax.axis_index("grp")
    wide = lax.axis_index("wide")
    z = lax.div(wide, 16)
    x_hi = lax.rem(lax.div(wide, 8), 2)
    y = lax.rem(lax.div(wide, 2), 4)
    core = lax.rem(wide, 2)
    x = 2 * x_hi + x_lo
    device_index = x_lo * 64 + wide

    def shift(v, by):
        return lax.rem(v + (by % 4), 4)

    def device(xx, yy, zz, cc):
        return (lax.rem(xx, 2), zz * 16 + lax.div(xx, 2) * 8 + yy * 2 + cc)

    xn, xf, xb = shift(x, 1), shift(x, 2), shift(x, -1)
    yn, yf, yb = shift(y, 1), shift(y, 2), shift(y, -1)
    zn, zf, zb = shift(z, 1), shift(z, 2), shift(z, -1)
    z_on, z_off = (lax.rem(z + 4 + s, 4) for s in (1 - 2 * core, 2 * core - 1))
    x_next, x_far, x_back = (device(v, y, z, core) for v in (xn, xf, xb))
    y_next, y_back = (device(x, v, z, core) for v in (yn, yb))
    z_next, z_back = (device(x, y, v, core) for v in (zn, zb))
    z_ring = device(x, y, z_on, core)
    partner = device(x, y, z, 1 - core)

    def feature_quarter(xx):
        return 2 * lax.rem(xx, 2) + lax.div(xx, 2)

    def q_cols(xx):
        return pl.ds(pl.multiple_of(feature_quarter(xx) * quarter, quarter), quarter)

    def slot(xx, cc):
        return pl.ds(pl.multiple_of((2 * xx + cc) * tokens, tokens), tokens)

    def chip_slot(xx):
        return pl.ds(pl.multiple_of(xx * chip_tokens, chip_tokens), chip_tokens)

    def rows_of(yy):
        return pl.ds(pl.multiple_of(yy * pair_rows, pair_rows), pair_rows)

    def low_rows_of(yy):
        return pl.ds(pl.multiple_of(yy * pair_rows, own_rows), own_rows)

    def high_rows_of(yy):
        return pl.ds(pl.multiple_of(yy * pair_rows + own_rows, own_rows), own_rows)

    def owner_rows(xh):
        return pl.ds(pl.multiple_of(y * pair_rows + xh * own_rows, own_rows), own_rows)

    cols_a = pl.ds(0, half)
    cols_b = pl.ds(half, half)
    all_p = pl.ds(0, 3)
    wire = Wire(send_sems, recv_sems)
    locals_used = [0]

    def fetch(src, dst):
        copy = pltpu.make_async_copy(src, dst, local_sems.at[locals_used[0]])
        locals_used[0] += 1
        copy.start()
        return copy

    ids_here = fetch(ids, ids_v)
    far_pool = fetch(pool.at[:, q_cols(xf)], pool_q.at[0])

    barrier = pltpu.get_barrier_semaphore()
    for peer in (x_next, x_back, x_far, y_next, y_back, z_next, z_back, partner):
        pl.semaphore_signal(barrier, inc=1, device_id=peer, device_id_type=MESH)
    pl.semaphore_wait(barrier, 8)

    x_hi_cols = pl.ds(pl.multiple_of(x_hi * quarter, quarter), quarter)
    other_cols = pl.ds(pl.multiple_of((1 - x_hi) * quarter, quarter), quarter)
    wx_pair = wire.send(
        gate_up.at[:, :, other_cols], weights.at[z, pl.ds(0, 2), owner_rows(x_hi), :], x_far
    )
    wx_down = wire.send(down.at[:, other_cols], weights.at[z, 2, owner_rows(x_hi), :], x_far)
    w_pair = fetch(gate_up.at[:, :, x_hi_cols], weights.at[z, pl.ds(0, 2), owner_rows(x_hi), :])
    w_down = fetch(down.at[:, x_hi_cols], weights.at[z, 2, owner_rows(x_hi), :])

    c_via = wire.send(cot.at[:, q_cols(xf)], via_c, x_back)
    early, late = pl.ds(0, tokens // 2), pl.ds(tokens // 2, tokens // 2)

    def half_slot(part_index):
        start = (2 * x + core) * tokens + part_index * (tokens // 2)
        return pl.ds(pl.multiple_of(start, tokens // 2), tokens // 2)

    c_next_a = wire.send(cot.at[early, q_cols(xn)], tok_c.at[half_slot(0), :], x_next)
    c_back = wire.send(cot.at[:, q_cols(xb)], tok_c.at[slot(x, core), :], x_back)
    c_own = fetch(cot.at[:, q_cols(x)], tok_c.at[slot(x, core), :])
    next_pool = fetch(pool.at[:, q_cols(xn)], pool_q.at[1])
    back_pool = fetch(pool.at[:, q_cols(xb)], pool_q.at[2])
    own_pool = fetch(pool.at[:, q_cols(x)], pool_q.at[3])

    ids_here.wait()
    local_ids = ids_v[...] - device_index * pool_rows
    row_ids = lax.broadcasted_iota(jnp.int32, (pool_rows, tokens), 0)
    chosen = jnp.where(row_ids == local_ids, 1.0, 0.0).astype(F32).T.astype(BF16)

    def pick(index, target, row_slot):
        def step(n, carry):
            cols = pl.ds(pl.multiple_of(n * tile, tile), tile)
            target[row_slot, cols] = dot_nn(chosen, pool_q[index, :, cols]).astype(BF16)
            return carry

        lax.fori_loop(0, quarter // tile, step, 0)

    every = pl.ds(0, tokens)
    far_pool.wait()
    pick(0, picked.at[0], every)
    x_via = wire.send(picked.at[0], via_x, x_next)
    c_next_b = wire.send(cot.at[late, q_cols(xn)], tok_c.at[half_slot(1), :], x_next)

    w_pair.wait()
    w_down.wait()
    wx_pair.wait_recv()
    wx_down.wait_recv()

    def w_block(zz, rows, cols):
        return weights.at[zz, all_p, rows, cols]

    def same(view, device_):
        return wire.send(view, view, device_)

    a_next = same(w_block(z, rows_of(y), cols_a), y_next)
    a_back = same(w_block(z, rows_of(y), cols_a), y_back)
    b_next = same(w_block(z, rows_of(y), cols_b), z_next)
    b_back = same(w_block(z, rows_of(y), cols_b), z_back)

    own_pool.wait()
    pick(3, tok_x, slot(x, core))
    dd_own_x = same(tok_x.at[slot(x, core), :], partner)
    c_own.wait()
    dd_own_c = same(tok_c.at[slot(x, core), :], partner)
    next_pool.wait()
    pick(1, picked.at[1], every)
    back_pool.wait()
    pick(2, picked.at[2], every)

    a_next.wait_recv()
    a_on = same(w_block(z, low_rows_of(yb), cols_a), y_next)
    a_back.wait_recv()
    a_off = same(w_block(z, high_rows_of(yn), cols_a), y_back)
    b_next.wait_recv()
    b_on = same(w_block(zb, low_rows_of(y), cols_b), z_next)
    b_back.wait_recv()
    b_off = same(w_block(zn, high_rows_of(y), cols_b), z_back)

    a_on.wait_recv()
    a_off.wait_recv()
    every_row = pl.ds(0, chunk_rows)
    lower, upper = pl.ds(0, chunk_rows // 2), pl.ds(chunk_rows // 2, chunk_rows // 2)
    a2_next = same(w_block(z, every_row, cols_a), z_next)
    a2_back = same(w_block(z, every_row, cols_a), z_back)
    b_on.wait_recv()
    b_off.wait_recv()
    b2_next = same(w_block(pl.ds(0, 4), rows_of(y), cols_b), y_next)
    b2_back = same(w_block(pl.ds(0, 4), rows_of(y), cols_b), y_back)

    c_via.wait_recv()
    c_pass = wire.send(via_c, tok_c.at[slot(xn, core), :], x_back)
    x_back_copy = wire.send(picked.at[2], tok_x.at[slot(x, core), :], x_back)
    x_via.wait_recv()
    x_pass = wire.send(via_x, tok_x.at[slot(xb, core), :], x_next)
    x_next_copy = wire.send(picked.at[1], tok_x.at[slot(x, core), :], x_next)

    c_back.wait_recv()
    dd_c_n = same(tok_c.at[slot(xn, core), :], partner)
    c_next_a.wait_recv()
    c_next_b.wait_recv()
    dd_c_b = same(tok_c.at[slot(xb, core), :], partner)

    a2_next.wait_recv()
    a2_on = same(w_block(zb, lower, cols_a), z_next)
    a2_back.wait_recv()
    a2_off = same(w_block(zn, upper, cols_a), z_back)
    b2_next.wait_recv()
    b2_on = same(w_block(pl.ds(0, 2), rows_of(yb), cols_b), y_next)
    b2_back.wait_recv()
    b2_off = same(w_block(pl.ds(2, 2), rows_of(yn), cols_b), y_back)

    c_pass.wait_recv()
    dd_c_f = same(tok_c.at[slot(xf, core), :], partner)
    x_pass.wait_recv()
    dd_x_f = same(tok_x.at[slot(xf, core), :], partner)

    for copy in (a2_on, a2_off, b2_on, b2_off):
        copy.wait_recv()

    def forward(xx, target):
        def step(j, carry):
            tx = tok_x[chip_slot(xx), :]
            for h in range(2):
                pair = weights[2 * j + h, 0:2].reshape(2 * chunk_rows, quarter)
                target[2 * j + h, :, 0 : 2 * chunk_rows] = dot_nt(tx, pair).astype(target.dtype)
            tc = tok_c[chip_slot(xx), :]
            both = weights[pl.ds(2 * j, 2), 2].reshape(2 * chunk_rows, quarter)
            back = dot_nt(tc, both).astype(target.dtype)
            target[2 * j, :, 2 * chunk_rows :] = back[:, :chunk_rows]
            target[2 * j + 1, :, 2 * chunk_rows :] = back[:, chunk_rows:]
            return carry

        lax.fori_loop(0, 2, step, 0)

    first, second = pl.ds(0, tokens), pl.ds(tokens, tokens)
    dd_c_f.wait_recv()
    dd_x_f.wait_recv()
    forward(xf, part.at[xf])
    order = (z_off, zf, z_on, z)
    rs1 = []
    for zz in order:
        rs1.append(
            (
                wire.send(part.at[xf, zz, first, :], r1p.at[zz], x_next),
                wire.send(part.at[xf, zz, second, :], r1m.at[zz], x_back),
            )
        )
    dd_own_x.wait_recv()
    dd_own_c.wait_recv()
    forward(x, part_own)

    x_back_copy.wait_recv()
    dd_x_n = same(tok_x.at[slot(xn, core), :], partner)
    x_next_copy.wait_recv()
    dd_x_b = same(tok_x.at[slot(xb, core), :], partner)
    dd_c_n.wait_recv()
    dd_x_n.wait_recv()
    forward(xn, part.at[xn])
    dd_c_b.wait_recv()
    dd_x_b.wait_recv()
    forward(xb, part.at[xb])

    def add_into(ref, *others):
        total = ref[...].astype(F32)
        for other in others:
            total = total + other[...].astype(F32)
        ref[...] = total.astype(ref.dtype)

    def own_lanes(xx):
        return pl.ds(pl.multiple_of(xx * chip_tokens, chip_tokens), chip_tokens)

    def low_lanes(xx):
        return pl.ds(pl.multiple_of(xx * chip_tokens, tokens), tokens)

    def high_lanes(xx):
        return pl.ds(pl.multiple_of(xx * chip_tokens + tokens, tokens), tokens)

    level = exponent[0]
    unscale = jnp.float32(0.0)
    for power in range(16):
        unscale = jnp.where(level == power, jnp.float32(0.5**power), unscale)

    every_unit = pl.ds(0, chunk_rows)
    rs2, ag, passed, yb1, yb2 = {}, {}, {}, {}, {}

    def reduce_on(k):
        zz = order[k]
        rs1[k][0].wait_recv()
        add_into(part.at[xn, zz, first, :], r1p.at[zz])
        fwd = wire.send(part.at[xn, zz], r2p.at[zz], x_next)
        rs1[k][1].wait_recv()
        add_into(part.at[xb, zz, second, :], r1m.at[zz])
        rs2[k] = (fwd, wire.send(part.at[xb, zz], r2m.at[zz], x_back))

    def activate(k):
        zz = order[k]
        rs2[k][0].wait_recv()
        rs2[k][1].wait_recv()
        total = part_own[zz] + r2p[zz].astype(F32) + r2m[zz].astype(F32)
        gate = total[:, :chunk_rows]
        up = total[:, chunk_rows : 2 * chunk_rows]
        delta = unscale * total[:, 2 * chunk_rows :]
        sig = 1.0 / (1.0 + jnp.exp(-gate))
        hidden = gate * sig * up
        delta_gate = delta * up * sig * (1.0 + gate * (1.0 - sig))
        delta_up = delta * gate * sig
        deltas[zz, 0, :, own_lanes(x)] = delta_gate.T.astype(BF16)
        deltas[zz, 1, :, own_lanes(x)] = delta_up.T.astype(BF16)
        deltas[zz, 2, :, own_lanes(x)] = hidden.T.astype(BF16)

    def gather(k):
        zz = order[k]
        low = deltas.at[zz, all_p, every_unit, low_lanes(x)]
        high = deltas.at[zz, all_p, every_unit, high_lanes(x)]
        early = (same(low, x_next), same(high, x_back))
        ag[k] = (early, (same(high, x_next), same(low, x_back)))

    def pass_on(k):
        zz = order[k]
        ag[k][0][0].wait_recv()
        on = same(deltas.at[zz, all_p, every_unit, low_lanes(xb)], x_next)
        ag[k][0][1].wait_recv()
        passed[k] = (on, same(deltas.at[zz, all_p, every_unit, high_lanes(xn)], x_back))

    def gathered(k):
        ag[k][1][0].wait_recv()
        ag[k][1][1].wait_recv()
        passed[k][0].wait_recv()
        passed[k][1].wait_recv()

    def grad_half(k, start, size):
        zz = order[k]

        def step(n, carry):
            cols = pl.ds(pl.multiple_of(start + n * tile, tile), tile)
            pair = deltas[zz, 0:2].reshape(2 * chunk_rows, 4 * chip_tokens)
            out = dot_nn(pair, tok_x[:, cols]).astype(BF16)
            grads[zz, 0, :, cols] = out[:chunk_rows]
            grads[zz, 1, :, cols] = out[chunk_rows:]
            down_part = unscale * dot_nn(deltas[zz, 2], tok_c[:, cols])
            grads[zz, 2, :, cols] = down_part.astype(BF16)
            return carry

        lax.fori_loop(0, size // tile, step, 0)

    cols_a, cols_b = pl.ds(0, part_a), pl.ds(part_a, part_b)

    def g_block(zz, rows, cols):
        return grads.at[zz, all_p, rows, cols]

    def add3(out, *terms):
        for p in range(3):
            total = terms[0][p].astype(F32)
            for term in terms[1:]:
                total = total + term[p].astype(F32)
            out[p] = total.astype(out.dtype)

    ring_of_a, ring_of_b = [], []

    def a_step(k):
        view = g_block(order[k], every_row, cols_a)
        if k > 0:
            ring_of_a[k - 1].wait_recv()
            add3(view, view, ring_a.at[k - 1])
        ring_of_a.append(wire.send(view, ring_a.at[k], z_ring))

    def b_step(k):
        view = sum_b.at[order[k]]
        if k > 0:
            ring_of_b[k - 1].wait_recv()
            add3(view, view, ring_b.at[k - 1])
        ring_of_b.append(wire.send(view, ring_b.at[k], z_ring))

    def b_first(k):
        zz = order[k]
        yb1[k] = (
            wire.send(g_block(zz, low_rows_of(yf), cols_b), yb1p.at[zz], y_next),
            wire.send(g_block(zz, high_rows_of(yf), cols_b), yb1m.at[zz], y_back),
        )

    def b_second(k):
        zz = order[k]
        yb1[k][0].wait_recv()
        view = g_block(zz, low_rows_of(yn), cols_b)
        add3(view, view, yb1p.at[zz])
        on = wire.send(g_block(zz, rows_of(yn), cols_b), yb2p.at[zz], y_next)
        yb1[k][1].wait_recv()
        view = g_block(zz, high_rows_of(yb), cols_b)
        add3(view, view, yb1m.at[zz])
        yb2[k] = (on, wire.send(g_block(zz, rows_of(yb), cols_b), yb2m.at[zz], y_back))

    def b_sum(k):
        zz = order[k]
        yb2[k][0].wait_recv()
        yb2[k][1].wait_recv()
        add3(sum_b.at[zz], g_block(zz, rows_of(y), cols_b), yb2p.at[zz], yb2m.at[zz])

    reduce_on(0)
    reduce_on(1)
    activate(0)
    gather(0)
    reduce_on(2)
    activate(1)
    pass_on(0)
    gather(1)
    reduce_on(3)
    activate(2)

    gathered(0)
    grad_half(0, 0, part_a)
    a_step(0)
    pass_on(1)
    gather(2)
    grad_half(0, part_a, part_b)
    b_first(0)
    b_second(0)
    activate(3)

    gathered(1)
    grad_half(1, 0, part_a)
    a_step(1)
    pass_on(2)
    gather(3)
    grad_half(1, part_a, part_b)
    b_first(1)
    b_sum(0)
    b_step(0)

    gathered(2)
    grad_half(2, 0, part_a)
    b_second(1)
    pass_on(3)
    grad_half(2, part_a, part_b)
    b_first(2)
    a_step(2)

    gathered(3)
    grad_half(3, part_a, part_b)
    b_first(3)
    b_second(2)
    b_sum(1)
    b_step(1)
    grad_half(3, 0, part_a)
    ring_of_a[2].wait_recv()
    add3(sum_a, g_block(z, every_row, cols_a), ring_a.at[2])

    def a_block(rows):
        return sum_a.at[all_p, rows, :]

    ya1 = (
        wire.send(a_block(low_rows_of(yf)), ya1p, y_next),
        wire.send(a_block(high_rows_of(yf)), ya1m, y_back),
    )
    b_second(3)
    b_sum(2)
    b_step(2)
    ya1[0].wait_recv()
    view = a_block(low_rows_of(yn))
    add3(view, view, ya1p)
    ya2_next = wire.send(a_block(rows_of(yn)), ya2p, y_next)
    ya1[1].wait_recv()
    view = a_block(high_rows_of(yb))
    add3(view, view, ya1m)
    ya2_back = wire.send(a_block(rows_of(yb)), ya2m, y_back)
    b_sum(3)
    ring_of_b[2].wait_recv()
    every_pair = pl.ds(0, pair_rows)
    add3(final.at[all_p, every_pair, cols_b], sum_b.at[z], ring_b.at[2])
    kept = pl.ds(pl.multiple_of(x_hi * own_rows, own_rows), own_rows)
    given = pl.ds(pl.multiple_of((1 - x_hi) * own_rows, own_rows), own_rows)
    every_own = pl.ds(0, own_rows)
    last_b = wire.send(
        final.at[all_p, given, cols_b], crossed.at[all_p, every_own, cols_b], x_far
    )
    ya2_next.wait_recv()
    ya2_back.wait_recv()
    add3(final.at[all_p, every_pair, cols_a], a_block(rows_of(y)), ya2p, ya2m)
    last_a = wire.send(
        final.at[all_p, given, cols_a], crossed.at[all_p, every_own, cols_a], x_far
    )
    out_pair[:, :, x_hi_cols] = final[0:2, kept, :]
    out_down[:, x_hi_cols] = final[2, kept, :]
    last_b.wait_recv()
    last_a.wait_recv()
    out_pair[:, :, other_cols] = crossed[0:2]
    out_down[:, other_cols] = crossed[2]
    wire.drain()


def per_device(x_pool, token_ids, cotangent, gate_up, down_weight, loss_exponent):
    tokens, width = cotangent.shape
    quarter = width // 4
    half = quarter // 2
    own_rows = down_weight.shape[0]
    pair_rows, chunk_rows = 2 * own_rows, 8 * own_rows
    chip_tokens, ring_tokens = 2 * tokens, 8 * tokens
    acts = 3 * chunk_rows
    part_a, part_b = split_columns(quarter)

    def held(*shape, dtype=BF16):
        return pltpu.VMEM(shape, dtype)

    scratch = [
        held(ring_tokens, quarter), held(ring_tokens, quarter),
        held(tokens, quarter), held(tokens, quarter),
        held(3, tokens, quarter), held(4, x_pool.shape[0], quarter),
        held(4, 3, chunk_rows, quarter),
        held(4, 4, chip_tokens, acts), held(4, chip_tokens, acts, dtype=F32),
        held(4, tokens, acts), held(4, tokens, acts),
        held(4, chip_tokens, acts), held(4, chip_tokens, acts),
        held(4, 3, chunk_rows, ring_tokens),
        held(4, 3, chunk_rows, quarter),
        held(3, 3, chunk_rows, part_a), held(3, chunk_rows, part_a),
        held(3, own_rows, part_a), held(3, own_rows, part_a),
        held(3, pair_rows, part_a), held(3, pair_rows, part_a),
        held(4, 3, own_rows, part_b), held(4, 3, own_rows, part_b),
        held(4, 3, pair_rows, part_b), held(4, 3, pair_rows, part_b),
        held(4, 3, pair_rows, part_b), held(3, 3, pair_rows, part_b),
        held(3, pair_rows, quarter), held(3, own_rows, quarter),
        pltpu.VMEM((1, tokens), jnp.int32),
        pltpu.SemaphoreType.DMA((SENDS,)),
        pltpu.SemaphoreType.DMA((COPIES,)),
        pltpu.SemaphoreType.DMA((LOCALS,)),
    ]
    far = pl.BlockSpec(memory_space=pltpu.HBM)
    near = pl.BlockSpec(memory_space=pltpu.VMEM)
    return pl.pallas_call(
        kernel,
        out_shape=(
            jax.ShapeDtypeStruct(gate_up.shape, BF16),
            jax.ShapeDtypeStruct(down_weight.shape, BF16),
        ),
        in_specs=[far, far, far, far, far, pl.BlockSpec(memory_space=pltpu.SMEM)],
        out_specs=(near, near),
        scratch_shapes=scratch,
        compiler_params=pltpu.CompilerParams(
            collective_id=0, has_side_effects=True, vmem_limit_bytes=56_000_000
        ),
    )(x_pool, token_ids.reshape(1, tokens), cotangent, gate_up, down_weight, loss_exponent)


def solution(mesh):
    in_specs = (
        P(("grp", "wide"), None),
        P(("grp", "wide")),
        P(("grp", "wide"), None),
        P(None, "wide", "grp"),
        P("wide", "grp"),
        P(),
    )
    out_specs = (P(None, "wide", "grp"), P("wide", "grp"))
    return jax.shard_map(
        per_device, mesh=mesh, in_specs=in_specs, out_specs=out_specs, check_vma=False
    )
```

```python
import functools

import jax
import jax.numpy as jnp
from jax import lax
from jax.experimental import pallas as pl
from jax.experimental.pallas import tpu as pltpu
from jax.sharding import PartitionSpec as P

MESH = pl.DeviceIdType.MESH
BF16 = jnp.bfloat16
F32 = jnp.float32
COPIES = 103
SENDS = 24
LOCALS = 8
TILE = 256


def dot_nt(a, b):
    return lax.dot_general(a, b, (((1,), (1,)), ((), ())), preferred_element_type=F32)


def dot_nn(a, b):
    return lax.dot_general(a, b, (((1,), (0,)), ((), ())), preferred_element_type=F32)


def split_columns(quarter):
    tiles = quarter // TILE
    low = max(1, 3 * tiles // 7)
    return low * TILE, (tiles - low) * TILE


class Wire:
    def __init__(self, send_sems, recv_sems):
        self.send_sems, self.recv_sems = send_sems, recv_sems
        self.count = 0
        self.sent = []

    def send(self, src, dst, device):
        lane = self.count % SENDS
        if self.count >= SENDS:
            self.sent[self.count - SENDS].wait_send()
        copy = pltpu.make_async_remote_copy(
            src_ref=src,
            dst_ref=dst,
            send_sem=self.send_sems.at[lane],
            recv_sem=self.recv_sems.at[self.count],
            device_id=device,
            device_id_type=MESH,
        )
        self.count += 1
        copy.start()
        self.sent.append(copy)
        return copy

    def drain(self):
        for copy in self.sent[-SENDS:]:
            copy.wait_send()


def kernel(
    pool, ids, cot, gate_up, down, exponent,
    out_pair, out_down,
    tok_x, tok_c, via_x, via_c, picked, pool_q, weights,
    part, part_own, r1p, r1m, r2p, r2m, deltas, grads,
    ring_a, sum_a, ya1p, ya1m, ya2p, ya2m,
    yb1p, yb1m, yb2p, yb2m, sum_b, ring_b,
    final, crossed, ids_v, send_sems, recv_sems, local_sems,
):
    tokens, width = cot.shape
    quarter = width // 4
    half = quarter // 2
    own_rows = down.shape[0]
    pair_rows = 2 * own_rows
    chunk_rows = 4 * pair_rows
    chip_tokens = 2 * tokens
    pool_rows = pool.shape[0]
    tile = TILE
    part_a, part_b = split_columns(quarter)

    x_lo = lax.axis_index("grp")
    wide = lax.axis_index("wide")
    z = lax.div(wide, 16)
    x_hi = lax.rem(lax.div(wide, 8), 2)
    y = lax.rem(lax.div(wide, 2), 4)
    core = lax.rem(wide, 2)
    x = 2 * x_hi + x_lo
    device_index = x_lo * 64 + wide

    def shift(v, by):
        return lax.rem(v + (by % 4), 4)

    def device(xx, yy, zz, cc):
        return (lax.rem(xx, 2), zz * 16 + lax.div(xx, 2) * 8 + yy * 2 + cc)

    xn, xf, xb = shift(x, 1), shift(x, 2), shift(x, -1)
    yn, yf, yb = shift(y, 1), shift(y, 2), shift(y, -1)
    zn, zf, zb = shift(z, 1), shift(z, 2), shift(z, -1)
    z_on, z_off = (lax.rem(z + 4 + s, 4) for s in (1 - 2 * core, 2 * core - 1))
    x_next, x_far, x_back = (device(v, y, z, core) for v in (xn, xf, xb))
    y_next, y_back = (device(x, v, z, core) for v in (yn, yb))
    z_next, z_back = (device(x, y, v, core) for v in (zn, zb))
    z_ring = device(x, y, z_on, core)
    partner = device(x, y, z, 1 - core)

    def feature_quarter(xx):
        return 2 * lax.rem(xx, 2) + lax.div(xx, 2)

    def q_cols(xx):
        return pl.ds(pl.multiple_of(feature_quarter(xx) * quarter, quarter), quarter)

    def slot(xx, cc):
        return pl.ds(pl.multiple_of((2 * xx + cc) * tokens, tokens), tokens)

    def chip_slot(xx):
        return pl.ds(pl.multiple_of(xx * chip_tokens, chip_tokens), chip_tokens)

    def rows_of(yy):
        return pl.ds(pl.multiple_of(yy * pair_rows, pair_rows), pair_rows)

    def low_rows_of(yy):
        return pl.ds(pl.multiple_of(yy * pair_rows, own_rows), own_rows)

    def high_rows_of(yy):
        return pl.ds(pl.multiple_of(yy * pair_rows + own_rows, own_rows), own_rows)

    def owner_rows(xh):
        return pl.ds(pl.multiple_of(y * pair_rows + xh * own_rows, own_rows), own_rows)

    cols_a = pl.ds(0, half)
    cols_b = pl.ds(half, half)
    all_p = pl.ds(0, 3)
    wire = Wire(send_sems, recv_sems)
    locals_used = [0]

    def fetch(src, dst):
        copy = pltpu.make_async_copy(src, dst, local_sems.at[locals_used[0]])
        locals_used[0] += 1
        copy.start()
        return copy

    ids_here = fetch(ids, ids_v)
    far_pool = fetch(pool.at[:, q_cols(xf)], pool_q.at[0])

    barrier = pltpu.get_barrier_semaphore()
    for peer in (x_next, x_back, x_far, y_next, y_back, z_next, z_back, partner):
        pl.semaphore_signal(barrier, inc=1, device_id=peer, device_id_type=MESH)
    pl.semaphore_wait(barrier, 8)

    x_hi_cols = pl.ds(pl.multiple_of(x_hi * quarter, quarter), quarter)
    other_cols = pl.ds(pl.multiple_of((1 - x_hi) * quarter, quarter), quarter)
    wx_pair = wire.send(
        gate_up.at[:, :, other_cols], weights.at[z, pl.ds(0, 2), owner_rows(x_hi), :], x_far
    )
    wx_down = wire.send(down.at[:, other_cols], weights.at[z, 2, owner_rows(x_hi), :], x_far)
    w_pair = fetch(gate_up.at[:, :, x_hi_cols], weights.at[z, pl.ds(0, 2), owner_rows(x_hi), :])
    w_down = fetch(down.at[:, x_hi_cols], weights.at[z, 2, owner_rows(x_hi), :])

    c_via = wire.send(cot.at[:, q_cols(xf)], via_c, x_back)
    early, late = pl.ds(0, tokens // 2), pl.ds(tokens // 2, tokens // 2)

    def half_slot(part_index):
        start = (2 * x + core) * tokens + part_index * (tokens // 2)
        return pl.ds(pl.multiple_of(start, tokens // 2), tokens // 2)

    c_next_a = wire.send(cot.at[early, q_cols(xn)], tok_c.at[half_slot(0), :], x_next)
    c_back = wire.send(cot.at[:, q_cols(xb)], tok_c.at[slot(x, core), :], x_back)
    c_own = fetch(cot.at[:, q_cols(x)], tok_c.at[slot(x, core), :])
    next_pool = fetch(pool.at[:, q_cols(xn)], pool_q.at[1])
    back_pool = fetch(pool.at[:, q_cols(xb)], pool_q.at[2])
    own_pool = fetch(pool.at[:, q_cols(x)], pool_q.at[3])

    ids_here.wait()
    local_ids = ids_v[...] - device_index * pool_rows
    row_ids = lax.broadcasted_iota(jnp.int32, (pool_rows, tokens), 0)
    chosen = jnp.where(row_ids == local_ids, 1.0, 0.0).astype(F32).T.astype(BF16)

    def pick(index, target, row_slot):
        def step(n, carry):
            cols = pl.ds(pl.multiple_of(n * tile, tile), tile)
            target[row_slot, cols] = dot_nn(chosen, pool_q[index, :, cols]).astype(BF16)
            return carry

        lax.fori_loop(0, quarter // tile, step, 0)

    every = pl.ds(0, tokens)
    far_pool.wait()
    pick(0, picked.at[0], every)
    x_via = wire.send(picked.at[0], via_x, x_next)
    c_next_b = wire.send(cot.at[late, q_cols(xn)], tok_c.at[half_slot(1), :], x_next)

    w_pair.wait()
    w_down.wait()
    wx_pair.wait_recv()
    wx_down.wait_recv()

    def w_block(zz, rows, cols):
        return weights.at[zz, all_p, rows, cols]

    def same(view, device_):
        return wire.send(view, view, device_)

    a_next = same(w_block(z, rows_of(y), cols_a), y_next)
    a_back = same(w_block(z, rows_of(y), cols_a), y_back)
    b_next = same(w_block(z, rows_of(y), cols_b), z_next)
    b_back = same(w_block(z, rows_of(y), cols_b), z_back)

    own_pool.wait()
    pick(3, tok_x, slot(x, core))
    dd_own_x = same(tok_x.at[slot(x, core), :], partner)
    c_own.wait()
    dd_own_c = same(tok_c.at[slot(x, core), :], partner)
    next_pool.wait()
    pick(1, picked.at[1], every)
    back_pool.wait()
    pick(2, picked.at[2], every)

    a_next.wait_recv()
    a_on = same(w_block(z, low_rows_of(yb), cols_a), y_next)
    a_back.wait_recv()
    a_off = same(w_block(z, high_rows_of(yn), cols_a), y_back)
    b_next.wait_recv()
    b_on = same(w_block(zb, low_rows_of(y), cols_b), z_next)
    b_back.wait_recv()
    b_off = same(w_block(zn, high_rows_of(y), cols_b), z_back)

    a_on.wait_recv()
    a_off.wait_recv()
    every_row = pl.ds(0, chunk_rows)
    lower, upper = pl.ds(0, chunk_rows // 2), pl.ds(chunk_rows // 2, chunk_rows // 2)
    a2_next = same(w_block(z, every_row, cols_a), z_next)
    a2_back = same(w_block(z, every_row, cols_a), z_back)
    b_on.wait_recv()
    b_off.wait_recv()
    b2_next = same(w_block(pl.ds(0, 4), rows_of(y), cols_b), y_next)
    b2_back = same(w_block(pl.ds(0, 4), rows_of(y), cols_b), y_back)

    c_via.wait_recv()
    c_pass = wire.send(via_c, tok_c.at[slot(xn, core), :], x_back)
    x_back_copy = wire.send(picked.at[2], tok_x.at[slot(x, core), :], x_back)
    x_via.wait_recv()
    x_pass = wire.send(via_x, tok_x.at[slot(xb, core), :], x_next)
    x_next_copy = wire.send(picked.at[1], tok_x.at[slot(x, core), :], x_next)

    c_back.wait_recv()
    dd_c_n = same(tok_c.at[slot(xn, core), :], partner)
    c_next_a.wait_recv()
    c_next_b.wait_recv()
    dd_c_b = same(tok_c.at[slot(xb, core), :], partner)

    a2_next.wait_recv()
    a2_on = same(w_block(zb, lower, cols_a), z_next)
    a2_back.wait_recv()
    a2_off = same(w_block(zn, upper, cols_a), z_back)
    b2_next.wait_recv()
    b2_on = same(w_block(pl.ds(0, 2), rows_of(yb), cols_b), y_next)
    b2_back.wait_recv()
    b2_off = same(w_block(pl.ds(2, 2), rows_of(yn), cols_b), y_back)

    c_pass.wait_recv()
    dd_c_f = same(tok_c.at[slot(xf, core), :], partner)
    x_pass.wait_recv()
    dd_x_f = same(tok_x.at[slot(xf, core), :], partner)

    for copy in (a2_on, a2_off, b2_on, b2_off):
        copy.wait_recv()

    def forward(xx, target):
        def step(j, carry):
            tx = tok_x[chip_slot(xx), :]
            for h in range(2):
                pair = weights[2 * j + h, 0:2].reshape(2 * chunk_rows, quarter)
                target[2 * j + h, :, 0 : 2 * chunk_rows] = dot_nt(tx, pair).astype(target.dtype)
            tc = tok_c[chip_slot(xx), :]
            both = weights[pl.ds(2 * j, 2), 2].reshape(2 * chunk_rows, quarter)
            back = dot_nt(tc, both).astype(target.dtype)
            target[2 * j, :, 2 * chunk_rows :] = back[:, :chunk_rows]
            target[2 * j + 1, :, 2 * chunk_rows :] = back[:, chunk_rows:]
            return carry

        lax.fori_loop(0, 2, step, 0)

    first, second = pl.ds(0, tokens), pl.ds(tokens, tokens)
    dd_c_f.wait_recv()
    dd_x_f.wait_recv()
    forward(xf, part.at[xf])
    order = (z_off, zf, z_on, z)
    rs1 = []
    for zz in order:
        rs1.append(
            (
                wire.send(part.at[xf, zz, first, :], r1p.at[zz], x_next),
                wire.send(part.at[xf, zz, second, :], r1m.at[zz], x_back),
            )
        )
    dd_own_x.wait_recv()
    dd_own_c.wait_recv()
    forward(x, part_own)

    x_back_copy.wait_recv()
    dd_x_n = same(tok_x.at[slot(xn, core), :], partner)
    x_next_copy.wait_recv()
    dd_x_b = same(tok_x.at[slot(xb, core), :], partner)
    dd_c_n.wait_recv()
    dd_x_n.wait_recv()
    forward(xn, part.at[xn])
    dd_c_b.wait_recv()
    dd_x_b.wait_recv()
    forward(xb, part.at[xb])

    def add_into(ref, *others):
        total = ref[...].astype(F32)
        for other in others:
            total = total + other[...].astype(F32)
        ref[...] = total.astype(ref.dtype)

    def own_lanes(xx):
        return pl.ds(pl.multiple_of(xx * chip_tokens, chip_tokens), chip_tokens)

    def low_lanes(xx):
        return pl.ds(pl.multiple_of(xx * chip_tokens, tokens), tokens)

    def high_lanes(xx):
        return pl.ds(pl.multiple_of(xx * chip_tokens + tokens, tokens), tokens)

    level = exponent[0]
    unscale = jnp.float32(0.0)
    for power in range(16):
        unscale = jnp.where(level == power, jnp.float32(0.5**power), unscale)

    every_unit = pl.ds(0, chunk_rows)
    rs2, ag, passed, yb1, yb2 = {}, {}, {}, {}, {}

    def reduce_on(k):
        zz = order[k]
        rs1[k][0].wait_recv()
        add_into(part.at[xn, zz, first, :], r1p.at[zz])
        fwd = wire.send(part.at[xn, zz], r2p.at[zz], x_next)
        rs1[k][1].wait_recv()
        add_into(part.at[xb, zz, second, :], r1m.at[zz])
        rs2[k] = (fwd, wire.send(part.at[xb, zz], r2m.at[zz], x_back))

    def activate(k):
        zz = order[k]
        rs2[k][0].wait_recv()
        rs2[k][1].wait_recv()
        total = part_own[zz] + r2p[zz].astype(F32) + r2m[zz].astype(F32)
        gate = total[:, :chunk_rows]
        up = total[:, chunk_rows : 2 * chunk_rows]
        delta = unscale * total[:, 2 * chunk_rows :]
        sig = 1.0 / (1.0 + jnp.exp(-gate))
        hidden = gate * sig * up
        delta_gate = delta * up * sig * (1.0 + gate * (1.0 - sig))
        delta_up = delta * gate * sig
        deltas[zz, 0, :, own_lanes(x)] = delta_gate.T.astype(BF16)
        deltas[zz, 1, :, own_lanes(x)] = delta_up.T.astype(BF16)
        deltas[zz, 2, :, own_lanes(x)] = hidden.T.astype(BF16)

    def gather(k):
        zz = order[k]
        low = deltas.at[zz, all_p, every_unit, low_lanes(x)]
        high = deltas.at[zz, all_p, every_unit, high_lanes(x)]
        early = (same(low, x_next), same(high, x_back))
        ag[k] = (early, (same(high, x_next), same(low, x_back)))

    def pass_on(k):
        zz = order[k]
        ag[k][0][0].wait_recv()
        on = same(deltas.at[zz, all_p, every_unit, low_lanes(xb)], x_next)
        ag[k][0][1].wait_recv()
        passed[k] = (on, same(deltas.at[zz, all_p, every_unit, high_lanes(xn)], x_back))

    def gathered(k):
        ag[k][1][0].wait_recv()
        ag[k][1][1].wait_recv()
        passed[k][0].wait_recv()
        passed[k][1].wait_recv()

    def grad_half(k, start, size):
        zz = order[k]

        def step(n, carry):
            cols = pl.ds(pl.multiple_of(start + n * tile, tile), tile)
            pair = deltas[zz, 0:2].reshape(2 * chunk_rows, 4 * chip_tokens)
            out = dot_nn(pair, tok_x[:, cols]).astype(BF16)
            grads[zz, 0, :, cols] = out[:chunk_rows]
            grads[zz, 1, :, cols] = out[chunk_rows:]
            down_part = unscale * dot_nn(deltas[zz, 2], tok_c[:, cols])
            grads[zz, 2, :, cols] = down_part.astype(BF16)
            return carry

        lax.fori_loop(0, size // tile, step, 0)

    cols_a, cols_b = pl.ds(0, part_a), pl.ds(part_a, part_b)

    def g_block(zz, rows, cols):
        return grads.at[zz, all_p, rows, cols]

    def add3(out, *terms):
        for p in range(3):
            total = terms[0][p].astype(F32)
            for term in terms[1:]:
                total = total + term[p].astype(F32)
            out[p] = total.astype(out.dtype)

    ring_of_a, ring_of_b = [], []

    def a_step(k):
        view = g_block(order[k], every_row, cols_a)
        if k > 0:
            ring_of_a[k - 1].wait_recv()
            add3(view, view, ring_a.at[k - 1])
        ring_of_a.append(wire.send(view, ring_a.at[k], z_ring))

    def b_step(k):
        view = sum_b.at[order[k]]
        if k > 0:
            ring_of_b[k - 1].wait_recv()
            add3(view, view, ring_b.at[k - 1])
        ring_of_b.append(wire.send(view, ring_b.at[k], z_ring))

    def b_first(k):
        zz = order[k]
        yb1[k] = (
            wire.send(g_block(zz, low_rows_of(yf), cols_b), yb1p.at[zz], y_next),
            wire.send(g_block(zz, high_rows_of(yf), cols_b), yb1m.at[zz], y_back),
        )

    def b_second(k):
        zz = order[k]
        yb1[k][0].wait_recv()
        view = g_block(zz, low_rows_of(yn), cols_b)
        add3(view, view, yb1p.at[zz])
        on = wire.send(g_block(zz, rows_of(yn), cols_b), yb2p.at[zz], y_next)
        yb1[k][1].wait_recv()
        view = g_block(zz, high_rows_of(yb), cols_b)
        add3(view, view, yb1m.at[zz])
        yb2[k] = (on, wire.send(g_block(zz, rows_of(yb), cols_b), yb2m.at[zz], y_back))

    def b_sum(k):
        zz = order[k]
        yb2[k][0].wait_recv()
        yb2[k][1].wait_recv()
        add3(sum_b.at[zz], g_block(zz, rows_of(y), cols_b), yb2p.at[zz], yb2m.at[zz])

    reduce_on(0)
    reduce_on(1)
    activate(0)
    gather(0)
    reduce_on(2)
    activate(1)
    pass_on(0)
    gather(1)
    reduce_on(3)
    activate(2)

    gathered(0)
    grad_half(0, 0, part_a)
    a_step(0)
    pass_on(1)
    gather(2)
    grad_half(0, part_a, part_b)
    b_first(0)
    b_second(0)
    activate(3)

    gathered(1)
    grad_half(1, 0, part_a)
    a_step(1)
    pass_on(2)
    gather(3)
    grad_half(1, part_a, part_b)
    b_first(1)
    b_sum(0)
    b_step(0)

    gathered(2)
    grad_half(2, 0, part_a)
    b_second(1)
    pass_on(3)
    grad_half(2, part_a, part_b)
    b_first(2)
    a_step(2)

    gathered(3)
    grad_half(3, part_a, part_b)
    b_first(3)
    b_second(2)
    b_sum(1)
    b_step(1)
    grad_half(3, 0, part_a)
    ring_of_a[2].wait_recv()
    add3(sum_a, g_block(z, every_row, cols_a), ring_a.at[2])

    def a_block(rows):
        return sum_a.at[all_p, rows, :]

    ya1 = (
        wire.send(a_block(low_rows_of(yf)), ya1p, y_next),
        wire.send(a_block(high_rows_of(yf)), ya1m, y_back),
    )
    b_second(3)
    b_sum(2)
    b_step(2)
    ya1[0].wait_recv()
    view = a_block(low_rows_of(yn))
    add3(view, view, ya1p)
    ya2_next = wire.send(a_block(rows_of(yn)), ya2p, y_next)
    ya1[1].wait_recv()
    view = a_block(high_rows_of(yb))
    add3(view, view, ya1m)
    ya2_back = wire.send(a_block(rows_of(yb)), ya2m, y_back)
    b_sum(3)
    ring_of_b[2].wait_recv()
    every_pair = pl.ds(0, pair_rows)
    add3(final.at[all_p, every_pair, cols_b], sum_b.at[z], ring_b.at[2])
    kept = pl.ds(pl.multiple_of(x_hi * own_rows, own_rows), own_rows)
    given = pl.ds(pl.multiple_of((1 - x_hi) * own_rows, own_rows), own_rows)
    every_own = pl.ds(0, own_rows)
    last_b = wire.send(
        final.at[all_p, given, cols_b], crossed.at[all_p, every_own, cols_b], x_far
    )
    ya2_next.wait_recv()
    ya2_back.wait_recv()
    add3(final.at[all_p, every_pair, cols_a], a_block(rows_of(y)), ya2p, ya2m)
    last_a = wire.send(
        final.at[all_p, given, cols_a], crossed.at[all_p, every_own, cols_a], x_far
    )
    out_pair[:, :, x_hi_cols] = final[0:2, kept, :]
    out_down[:, x_hi_cols] = final[2, kept, :]
    last_b.wait_recv()
    last_a.wait_recv()
    out_pair[:, :, other_cols] = crossed[0:2]
    out_down[:, other_cols] = crossed[2]
    wire.drain()


def per_device(x_pool, token_ids, cotangent, gate_up, down_weight, loss_exponent):
    tokens, width = cotangent.shape
    quarter = width // 4
    half = quarter // 2
    own_rows = down_weight.shape[0]
    pair_rows, chunk_rows = 2 * own_rows, 8 * own_rows
    chip_tokens, ring_tokens = 2 * tokens, 8 * tokens
    acts = 3 * chunk_rows
    part_a, part_b = split_columns(quarter)

    def held(*shape, dtype=BF16):
        return pltpu.VMEM(shape, dtype)

    scratch = [
        held(ring_tokens, quarter), held(ring_tokens, quarter),
        held(tokens, quarter), held(tokens, quarter),
        held(3, tokens, quarter), held(4, x_pool.shape[0], quarter),
        held(4, 3, chunk_rows, quarter),
        held(4, 4, chip_tokens, acts), held(4, chip_tokens, acts, dtype=F32),
        held(4, tokens, acts), held(4, tokens, acts),
        held(4, chip_tokens, acts), held(4, chip_tokens, acts),
        held(4, 3, chunk_rows, ring_tokens),
        held(4, 3, chunk_rows, quarter),
        held(3, 3, chunk_rows, part_a), held(3, chunk_rows, part_a),
        held(3, own_rows, part_a), held(3, own_rows, part_a),
        held(3, pair_rows, part_a), held(3, pair_rows, part_a),
        held(4, 3, own_rows, part_b), held(4, 3, own_rows, part_b),
        held(4, 3, pair_rows, part_b), held(4, 3, pair_rows, part_b),
        held(4, 3, pair_rows, part_b), held(3, 3, pair_rows, part_b),
        held(3, pair_rows, quarter), held(3, own_rows, quarter),
        pltpu.VMEM((1, tokens), jnp.int32),
        pltpu.SemaphoreType.DMA((SENDS,)),
        pltpu.SemaphoreType.DMA((COPIES,)),
        pltpu.SemaphoreType.DMA((LOCALS,)),
    ]
    far = pl.BlockSpec(memory_space=pltpu.HBM)
    near = pl.BlockSpec(memory_space=pltpu.VMEM)
    return pl.pallas_call(
        kernel,
        out_shape=(
            jax.ShapeDtypeStruct(gate_up.shape, BF16),
            jax.ShapeDtypeStruct(down_weight.shape, BF16),
        ),
        in_specs=[far, far, far, far, far, pl.BlockSpec(memory_space=pltpu.SMEM)],
        out_specs=(near, near),
        scratch_shapes=scratch,
        compiler_params=pltpu.CompilerParams(
            collective_id=0, has_side_effects=True, vmem_limit_bytes=56_000_000
        ),
    )(*[pltpu.with_memory_space_constraint(v, pltpu.HBM) for v in (x_pool, token_ids.reshape(1, tokens), cotangent, gate_up, down_weight)], loss_exponent)


def solution(mesh):
    in_specs = (
        P(("grp", "wide"), None),
        P(("grp", "wide")),
        P(("grp", "wide"), None),
        P(None, "wide", "grp"),
        P("wide", "grp"),
        P(),
    )
    out_specs = (P(None, "wide", "grp"), P("wide", "grp"))
    return jax.shard_map(
        per_device, mesh=mesh, in_specs=in_specs, out_specs=out_specs, check_vma=False
    )
```

```python
import functools

import jax
import jax.numpy as jnp
from jax import lax
from jax.experimental import pallas as pl
from jax.experimental.pallas import tpu as pltpu
from jax.sharding import PartitionSpec as P

MESH = pl.DeviceIdType.MESH
BF16 = jnp.bfloat16
F32 = jnp.float32
COPIES = 103
SENDS = 24
LOCALS = 8
TILE = 256


def dot_nt(a, b):
    return lax.dot_general(a, b, (((1,), (1,)), ((), ())), preferred_element_type=F32)


def dot_nn(a, b):
    return lax.dot_general(a, b, (((1,), (0,)), ((), ())), preferred_element_type=F32)


def split_columns(quarter):
    tiles = quarter // TILE
    low = max(1, 3 * tiles // 7)
    return low * TILE, (tiles - low) * TILE


class Wire:
    def __init__(self, send_sems, recv_sems):
        self.send_sems, self.recv_sems = send_sems, recv_sems
        self.count = 0
        self.sent = []

    def send(self, src, dst, device):
        lane = self.count % SENDS
        if self.count >= SENDS:
            self.sent[self.count - SENDS].wait_send()
        copy = pltpu.make_async_remote_copy(
            src_ref=src,
            dst_ref=dst,
            send_sem=self.send_sems.at[lane],
            recv_sem=self.recv_sems.at[self.count],
            device_id=device,
            device_id_type=MESH,
        )
        self.count += 1
        copy.start()
        self.sent.append(copy)
        return copy

    def drain(self):
        for copy in self.sent[-SENDS:]:
            copy.wait_send()


def kernel(
    pool, ids, cot, gate_up, down, exponent,
    out_pair, out_down,
    tok_x, tok_c, via_x, via_c, picked, pool_q, weights,
    part, part_own, r1p, r1m, r2p, r2m, deltas, grads,
    ring_a, sum_a, ya1p, ya1m, ya2p, ya2m,
    yb1p, yb1m, yb2p, yb2m, sum_b, ring_b,
    final, crossed, ids_v, send_sems, recv_sems, local_sems,
):
    tokens, width = cot.shape
    quarter = width // 4
    half = quarter // 2
    own_rows = down.shape[0]
    pair_rows = 2 * own_rows
    chunk_rows = 4 * pair_rows
    chip_tokens = 2 * tokens
    pool_rows = pool.shape[0]
    tile = TILE
    part_a, part_b = split_columns(quarter)

    x_lo = lax.axis_index("grp")
    wide = lax.axis_index("wide")
    z = lax.div(wide, 16)
    x_hi = lax.rem(lax.div(wide, 8), 2)
    y = lax.rem(lax.div(wide, 2), 4)
    core = lax.rem(wide, 2)
    x = 2 * x_hi + x_lo
    device_index = x_lo * 64 + wide

    def shift(v, by):
        return lax.rem(v + (by % 4), 4)

    def device(xx, yy, zz, cc):
        return (lax.rem(xx, 2), zz * 16 + lax.div(xx, 2) * 8 + yy * 2 + cc)

    xn, xf, xb = shift(x, 1), shift(x, 2), shift(x, -1)
    yn, yf, yb = shift(y, 1), shift(y, 2), shift(y, -1)
    zn, zf, zb = shift(z, 1), shift(z, 2), shift(z, -1)
    z_on, z_off = (lax.rem(z + 4 + s, 4) for s in (1 - 2 * core, 2 * core - 1))
    x_next, x_far, x_back = (device(v, y, z, core) for v in (xn, xf, xb))
    y_next, y_back = (device(x, v, z, core) for v in (yn, yb))
    z_next, z_back = (device(x, y, v, core) for v in (zn, zb))
    z_ring = device(x, y, z_on, core)
    partner = device(x, y, z, 1 - core)

    def feature_quarter(xx):
        return 2 * lax.rem(xx, 2) + lax.div(xx, 2)

    def q_cols(xx):
        return pl.ds(pl.multiple_of(feature_quarter(xx) * quarter, quarter), quarter)

    def slot(xx, cc):
        return pl.ds(pl.multiple_of((2 * xx + cc) * tokens, tokens), tokens)

    def chip_slot(xx):
        return pl.ds(pl.multiple_of(xx * chip_tokens, chip_tokens), chip_tokens)

    def rows_of(yy):
        return pl.ds(pl.multiple_of(yy * pair_rows, pair_rows), pair_rows)

    def low_rows_of(yy):
        return pl.ds(pl.multiple_of(yy * pair_rows, own_rows), own_rows)

    def high_rows_of(yy):
        return pl.ds(pl.multiple_of(yy * pair_rows + own_rows, own_rows), own_rows)

    def owner_rows(xh):
        return pl.ds(pl.multiple_of(y * pair_rows + xh * own_rows, own_rows), own_rows)

    cols_a = pl.ds(0, half)
    cols_b = pl.ds(half, half)
    all_p = pl.ds(0, 3)
    wire = Wire(send_sems, recv_sems)
    locals_used = [0]

    def fetch(src, dst):
        copy = pltpu.make_async_copy(src, dst, local_sems.at[locals_used[0]])
        locals_used[0] += 1
        copy.start()
        return copy

    ids_here = fetch(ids, ids_v)
    far_pool = fetch(pool.at[:, q_cols(xf)], pool_q.at[0])

    barrier = pltpu.get_barrier_semaphore()
    for peer in (x_next, x_back, x_far, y_next, y_back, z_next, z_back, partner):
        pl.semaphore_signal(barrier, inc=1, device_id=peer, device_id_type=MESH)
    pl.semaphore_wait(barrier, 8)

    x_hi_cols = pl.ds(pl.multiple_of(x_hi * quarter, quarter), quarter)
    other_cols = pl.ds(pl.multiple_of((1 - x_hi) * quarter, quarter), quarter)
    wx_pair = wire.send(
        gate_up.at[:, :, other_cols], weights.at[z, pl.ds(0, 2), owner_rows(x_hi), :], x_far
    )
    wx_down = wire.send(down.at[:, other_cols], weights.at[z, 2, owner_rows(x_hi), :], x_far)
    w_pair = fetch(gate_up.at[:, :, x_hi_cols], weights.at[z, pl.ds(0, 2), owner_rows(x_hi), :])
    w_down = fetch(down.at[:, x_hi_cols], weights.at[z, 2, owner_rows(x_hi), :])

    c_via = wire.send(cot.at[:, q_cols(xf)], via_c, x_back)
    early, late = pl.ds(0, tokens // 2), pl.ds(tokens // 2, tokens // 2)

    def half_slot(part_index):
        start = (2 * x + core) * tokens + part_index * (tokens // 2)
        return pl.ds(pl.multiple_of(start, tokens // 2), tokens // 2)

    c_next_a = wire.send(cot.at[early, q_cols(xn)], tok_c.at[half_slot(0), :], x_next)
    c_back = wire.send(cot.at[:, q_cols(xb)], tok_c.at[slot(x, core), :], x_back)
    c_own = fetch(cot.at[:, q_cols(x)], tok_c.at[slot(x, core), :])
    next_pool = fetch(pool.at[:, q_cols(xn)], pool_q.at[1])
    back_pool = fetch(pool.at[:, q_cols(xb)], pool_q.at[2])
    own_pool = fetch(pool.at[:, q_cols(x)], pool_q.at[3])

    ids_here.wait()
    local_ids = ids_v[...] - device_index * pool_rows
    row_ids = lax.broadcasted_iota(jnp.int32, (pool_rows, tokens), 0)
    chosen = jnp.where(row_ids == local_ids, 1.0, 0.0).astype(F32).T.astype(BF16)

    def pick(index, target, row_slot):
        def step(n, carry):
            cols = pl.ds(pl.multiple_of(n * tile, tile), tile)
            target[row_slot, cols] = dot_nn(chosen, pool_q[index, :, cols]).astype(BF16)
            return carry

        lax.fori_loop(0, quarter // tile, step, 0)

    every = pl.ds(0, tokens)
    far_pool.wait()
    pick(0, picked.at[0], every)
    x_via = wire.send(picked.at[0], via_x, x_next)
    c_next_b = wire.send(cot.at[late, q_cols(xn)], tok_c.at[half_slot(1), :], x_next)

    w_pair.wait()
    w_down.wait()
    wx_pair.wait_recv()
    wx_down.wait_recv()

    def w_block(zz, rows, cols):
        return weights.at[zz, all_p, rows, cols]

    def same(view, device_):
        return wire.send(view, view, device_)

    a_next = same(w_block(z, rows_of(y), cols_a), y_next)
    a_back = same(w_block(z, rows_of(y), cols_a), y_back)
    b_next = same(w_block(z, rows_of(y), cols_b), z_next)
    b_back = same(w_block(z, rows_of(y), cols_b), z_back)


    a_next.wait_recv()
    a_on = same(w_block(z, low_rows_of(yb), cols_a), y_next)
    a_back.wait_recv()
    a_off = same(w_block(z, high_rows_of(yn), cols_a), y_back)
    b_next.wait_recv()
    b_on = same(w_block(zb, low_rows_of(y), cols_b), z_next)
    b_back.wait_recv()
    b_off = same(w_block(zn, high_rows_of(y), cols_b), z_back)

    next_pool.wait()
    pick(1, picked.at[1], every)
    back_pool.wait()
    pick(2, picked.at[2], every)

    a_on.wait_recv()
    a_off.wait_recv()
    every_row = pl.ds(0, chunk_rows)
    lower, upper = pl.ds(0, chunk_rows // 2), pl.ds(chunk_rows // 2, chunk_rows // 2)
    a2_next = same(w_block(z, every_row, cols_a), z_next)
    a2_back = same(w_block(z, every_row, cols_a), z_back)
    b_on.wait_recv()
    b_off.wait_recv()
    b2_next = same(w_block(pl.ds(0, 4), rows_of(y), cols_b), y_next)
    b2_back = same(w_block(pl.ds(0, 4), rows_of(y), cols_b), y_back)

    c_via.wait_recv()
    c_pass = wire.send(via_c, tok_c.at[slot(xn, core), :], x_back)
    x_back_copy = wire.send(picked.at[2], tok_x.at[slot(x, core), :], x_back)
    x_via.wait_recv()
    x_pass = wire.send(via_x, tok_x.at[slot(xb, core), :], x_next)
    x_next_copy = wire.send(picked.at[1], tok_x.at[slot(x, core), :], x_next)

    own_pool.wait()
    pick(3, tok_x, slot(x, core))
    dd_own_x = same(tok_x.at[slot(x, core), :], partner)
    c_own.wait()
    dd_own_c = same(tok_c.at[slot(x, core), :], partner)
    c_back.wait_recv()
    dd_c_n = same(tok_c.at[slot(xn, core), :], partner)
    c_next_a.wait_recv()
    c_next_b.wait_recv()
    dd_c_b = same(tok_c.at[slot(xb, core), :], partner)

    a2_next.wait_recv()
    a2_on = same(w_block(zb, lower, cols_a), z_next)
    a2_back.wait_recv()
    a2_off = same(w_block(zn, upper, cols_a), z_back)
    b2_next.wait_recv()
    b2_on = same(w_block(pl.ds(0, 2), rows_of(yb), cols_b), y_next)
    b2_back.wait_recv()
    b2_off = same(w_block(pl.ds(2, 2), rows_of(yn), cols_b), y_back)

    c_pass.wait_recv()
    dd_c_f = same(tok_c.at[slot(xf, core), :], partner)
    x_pass.wait_recv()
    dd_x_f = same(tok_x.at[slot(xf, core), :], partner)

    for copy in (a2_on, a2_off, b2_on, b2_off):
        copy.wait_recv()

    def forward(xx, target):
        def step(j, carry):
            tx = tok_x[chip_slot(xx), :]
            for h in range(2):
                pair = weights[2 * j + h, 0:2].reshape(2 * chunk_rows, quarter)
                target[2 * j + h, :, 0 : 2 * chunk_rows] = dot_nt(tx, pair).astype(target.dtype)
            tc = tok_c[chip_slot(xx), :]
            both = weights[pl.ds(2 * j, 2), 2].reshape(2 * chunk_rows, quarter)
            back = dot_nt(tc, both).astype(target.dtype)
            target[2 * j, :, 2 * chunk_rows :] = back[:, :chunk_rows]
            target[2 * j + 1, :, 2 * chunk_rows :] = back[:, chunk_rows:]
            return carry

        lax.fori_loop(0, 2, step, 0)

    first, second = pl.ds(0, tokens), pl.ds(tokens, tokens)
    dd_c_f.wait_recv()
    dd_x_f.wait_recv()
    forward(xf, part.at[xf])
    order = (z_off, zf, z_on, z)
    rs1 = []
    for zz in order:
        rs1.append(
            (
                wire.send(part.at[xf, zz, first, :], r1p.at[zz], x_next),
                wire.send(part.at[xf, zz, second, :], r1m.at[zz], x_back),
            )
        )
    dd_own_x.wait_recv()
    dd_own_c.wait_recv()
    forward(x, part_own)

    x_back_copy.wait_recv()
    dd_x_n = same(tok_x.at[slot(xn, core), :], partner)
    x_next_copy.wait_recv()
    dd_x_b = same(tok_x.at[slot(xb, core), :], partner)
    dd_c_n.wait_recv()
    dd_x_n.wait_recv()
    forward(xn, part.at[xn])
    dd_c_b.wait_recv()
    dd_x_b.wait_recv()
    forward(xb, part.at[xb])

    def add_into(ref, *others):
        total = ref[...].astype(F32)
        for other in others:
            total = total + other[...].astype(F32)
        ref[...] = total.astype(ref.dtype)

    def own_lanes(xx):
        return pl.ds(pl.multiple_of(xx * chip_tokens, chip_tokens), chip_tokens)

    def low_lanes(xx):
        return pl.ds(pl.multiple_of(xx * chip_tokens, tokens), tokens)

    def high_lanes(xx):
        return pl.ds(pl.multiple_of(xx * chip_tokens + tokens, tokens), tokens)

    level = exponent[0]
    unscale = jnp.float32(0.0)
    for power in range(16):
        unscale = jnp.where(level == power, jnp.float32(0.5**power), unscale)

    every_unit = pl.ds(0, chunk_rows)
    rs2, ag, passed, yb1, yb2 = {}, {}, {}, {}, {}

    def reduce_on(k):
        zz = order[k]
        rs1[k][0].wait_recv()
        add_into(part.at[xn, zz, first, :], r1p.at[zz])
        fwd = wire.send(part.at[xn, zz], r2p.at[zz], x_next)
        rs1[k][1].wait_recv()
        add_into(part.at[xb, zz, second, :], r1m.at[zz])
        rs2[k] = (fwd, wire.send(part.at[xb, zz], r2m.at[zz], x_back))

    def activate(k):
        zz = order[k]
        rs2[k][0].wait_recv()
        rs2[k][1].wait_recv()
        total = part_own[zz] + r2p[zz].astype(F32) + r2m[zz].astype(F32)
        gate = total[:, :chunk_rows]
        up = total[:, chunk_rows : 2 * chunk_rows]
        delta = unscale * total[:, 2 * chunk_rows :]
        sig = 1.0 / (1.0 + jnp.exp(-gate))
        hidden = gate * sig * up
        delta_gate = delta * up * sig * (1.0 + gate * (1.0 - sig))
        delta_up = delta * gate * sig
        deltas[zz, 0, :, own_lanes(x)] = delta_gate.T.astype(BF16)
        deltas[zz, 1, :, own_lanes(x)] = delta_up.T.astype(BF16)
        deltas[zz, 2, :, own_lanes(x)] = hidden.T.astype(BF16)

    def gather(k):
        zz = order[k]
        low = deltas.at[zz, all_p, every_unit, low_lanes(x)]
        high = deltas.at[zz, all_p, every_unit, high_lanes(x)]
        early = (same(low, x_next), same(high, x_back))
        ag[k] = (early, (same(high, x_next), same(low, x_back)))

    def pass_on(k):
        zz = order[k]
        ag[k][0][0].wait_recv()
        on = same(deltas.at[zz, all_p, every_unit, low_lanes(xb)], x_next)
        ag[k][0][1].wait_recv()
        passed[k] = (on, same(deltas.at[zz, all_p, every_unit, high_lanes(xn)], x_back))

    def gathered(k):
        ag[k][1][0].wait_recv()
        ag[k][1][1].wait_recv()
        passed[k][0].wait_recv()
        passed[k][1].wait_recv()

    def grad_half(k, start, size):
        zz = order[k]

        def step(n, carry):
            cols = pl.ds(pl.multiple_of(start + n * tile, tile), tile)
            pair = deltas[zz, 0:2].reshape(2 * chunk_rows, 4 * chip_tokens)
            out = dot_nn(pair, tok_x[:, cols]).astype(BF16)
            grads[zz, 0, :, cols] = out[:chunk_rows]
            grads[zz, 1, :, cols] = out[chunk_rows:]
            down_part = unscale * dot_nn(deltas[zz, 2], tok_c[:, cols])
            grads[zz, 2, :, cols] = down_part.astype(BF16)
            return carry

        lax.fori_loop(0, size // tile, step, 0)

    cols_a, cols_b = pl.ds(0, part_a), pl.ds(part_a, part_b)

    def g_block(zz, rows, cols):
        return grads.at[zz, all_p, rows, cols]

    def add3(out, *terms):
        for p in range(3):
            total = terms[0][p].astype(F32)
            for term in terms[1:]:
                total = total + term[p].astype(F32)
            out[p] = total.astype(out.dtype)

    ring_of_a, ring_of_b = [], []

    def a_step(k):
        view = g_block(order[k], every_row, cols_a)
        if k > 0:
            ring_of_a[k - 1].wait_recv()
            add3(view, view, ring_a.at[k - 1])
        ring_of_a.append(wire.send(view, ring_a.at[k], z_ring))

    def b_step(k):
        view = sum_b.at[order[k]]
        if k > 0:
            ring_of_b[k - 1].wait_recv()
            add3(view, view, ring_b.at[k - 1])
        ring_of_b.append(wire.send(view, ring_b.at[k], z_ring))

    def b_first(k):
        zz = order[k]
        yb1[k] = (
            wire.send(g_block(zz, low_rows_of(yf), cols_b), yb1p.at[zz], y_next),
            wire.send(g_block(zz, high_rows_of(yf), cols_b), yb1m.at[zz], y_back),
        )

    def b_second(k):
        zz = order[k]
        yb1[k][0].wait_recv()
        view = g_block(zz, low_rows_of(yn), cols_b)
        add3(view, view, yb1p.at[zz])
        on = wire.send(g_block(zz, rows_of(yn), cols_b), yb2p.at[zz], y_next)
        yb1[k][1].wait_recv()
        view = g_block(zz, high_rows_of(yb), cols_b)
        add3(view, view, yb1m.at[zz])
        yb2[k] = (on, wire.send(g_block(zz, rows_of(yb), cols_b), yb2m.at[zz], y_back))

    def b_sum(k):
        zz = order[k]
        yb2[k][0].wait_recv()
        yb2[k][1].wait_recv()
        add3(sum_b.at[zz], g_block(zz, rows_of(y), cols_b), yb2p.at[zz], yb2m.at[zz])

    reduce_on(0)
    reduce_on(1)
    activate(0)
    gather(0)
    reduce_on(2)
    activate(1)
    pass_on(0)
    gather(1)
    reduce_on(3)
    activate(2)

    gathered(0)
    grad_half(0, 0, part_a)
    a_step(0)
    pass_on(1)
    gather(2)
    grad_half(0, part_a, part_b)
    b_first(0)
    b_second(0)
    activate(3)

    gathered(1)
    grad_half(1, 0, part_a)
    a_step(1)
    pass_on(2)
    gather(3)
    grad_half(1, part_a, part_b)
    b_first(1)
    b_sum(0)
    b_step(0)

    gathered(2)
    grad_half(2, 0, part_a)
    b_second(1)
    pass_on(3)
    grad_half(2, part_a, part_b)
    b_first(2)
    a_step(2)

    gathered(3)
    grad_half(3, part_a, part_b)
    b_first(3)
    b_second(2)
    b_sum(1)
    b_step(1)
    grad_half(3, 0, part_a)
    ring_of_a[2].wait_recv()
    add3(sum_a, g_block(z, every_row, cols_a), ring_a.at[2])

    def a_block(rows):
        return sum_a.at[all_p, rows, :]

    ya1 = (
        wire.send(a_block(low_rows_of(yf)), ya1p, y_next),
        wire.send(a_block(high_rows_of(yf)), ya1m, y_back),
    )
    b_second(3)
    b_sum(2)
    b_step(2)
    ya1[0].wait_recv()
    view = a_block(low_rows_of(yn))
    add3(view, view, ya1p)
    ya2_next = wire.send(a_block(rows_of(yn)), ya2p, y_next)
    ya1[1].wait_recv()
    view = a_block(high_rows_of(yb))
    add3(view, view, ya1m)
    ya2_back = wire.send(a_block(rows_of(yb)), ya2m, y_back)
    b_sum(3)
    ring_of_b[2].wait_recv()
    every_pair = pl.ds(0, pair_rows)
    add3(final.at[all_p, every_pair, cols_b], sum_b.at[z], ring_b.at[2])
    kept = pl.ds(pl.multiple_of(x_hi * own_rows, own_rows), own_rows)
    given = pl.ds(pl.multiple_of((1 - x_hi) * own_rows, own_rows), own_rows)
    every_own = pl.ds(0, own_rows)
    last_b = wire.send(
        final.at[all_p, given, cols_b], crossed.at[all_p, every_own, cols_b], x_far
    )
    ya2_next.wait_recv()
    ya2_back.wait_recv()
    add3(final.at[all_p, every_pair, cols_a], a_block(rows_of(y)), ya2p, ya2m)
    last_a = wire.send(
        final.at[all_p, given, cols_a], crossed.at[all_p, every_own, cols_a], x_far
    )
    out_pair[:, :, x_hi_cols] = final[0:2, kept, :]
    out_down[:, x_hi_cols] = final[2, kept, :]
    last_b.wait_recv()
    last_a.wait_recv()
    out_pair[:, :, other_cols] = crossed[0:2]
    out_down[:, other_cols] = crossed[2]
    wire.drain()


def per_device(x_pool, token_ids, cotangent, gate_up, down_weight, loss_exponent):
    tokens, width = cotangent.shape
    quarter = width // 4
    half = quarter // 2
    own_rows = down_weight.shape[0]
    pair_rows, chunk_rows = 2 * own_rows, 8 * own_rows
    chip_tokens, ring_tokens = 2 * tokens, 8 * tokens
    acts = 3 * chunk_rows
    part_a, part_b = split_columns(quarter)

    def held(*shape, dtype=BF16):
        return pltpu.VMEM(shape, dtype)

    scratch = [
        held(ring_tokens, quarter), held(ring_tokens, quarter),
        held(tokens, quarter), held(tokens, quarter),
        held(3, tokens, quarter), held(4, x_pool.shape[0], quarter),
        held(4, 3, chunk_rows, quarter),
        held(4, 4, chip_tokens, acts), held(4, chip_tokens, acts, dtype=F32),
        held(4, tokens, acts), held(4, tokens, acts),
        held(4, chip_tokens, acts), held(4, chip_tokens, acts),
        held(4, 3, chunk_rows, ring_tokens),
        held(4, 3, chunk_rows, quarter),
        held(3, 3, chunk_rows, part_a), held(3, chunk_rows, part_a),
        held(3, own_rows, part_a), held(3, own_rows, part_a),
        held(3, pair_rows, part_a), held(3, pair_rows, part_a),
        held(4, 3, own_rows, part_b), held(4, 3, own_rows, part_b),
        held(4, 3, pair_rows, part_b), held(4, 3, pair_rows, part_b),
        held(4, 3, pair_rows, part_b), held(3, 3, pair_rows, part_b),
        held(3, pair_rows, quarter), held(3, own_rows, quarter),
        pltpu.VMEM((1, tokens), jnp.int32),
        pltpu.SemaphoreType.DMA((SENDS,)),
        pltpu.SemaphoreType.DMA((COPIES,)),
        pltpu.SemaphoreType.DMA((LOCALS,)),
    ]
    far = pl.BlockSpec(memory_space=pltpu.HBM)
    near = pl.BlockSpec(memory_space=pltpu.VMEM)
    return pl.pallas_call(
        kernel,
        out_shape=(
            jax.ShapeDtypeStruct(gate_up.shape, BF16),
            jax.ShapeDtypeStruct(down_weight.shape, BF16),
        ),
        in_specs=[far, far, far, far, far, pl.BlockSpec(memory_space=pltpu.SMEM)],
        out_specs=(near, near),
        scratch_shapes=scratch,
        compiler_params=pltpu.CompilerParams(
            collective_id=0, has_side_effects=True, vmem_limit_bytes=56_000_000
        ),
    )(*[pltpu.with_memory_space_constraint(v, pltpu.HBM) for v in (x_pool, token_ids.reshape(1, tokens), cotangent, gate_up, down_weight)], loss_exponent)


def solution(mesh):
    in_specs = (
        P(("grp", "wide"), None),
        P(("grp", "wide")),
        P(("grp", "wide"), None),
        P(None, "wide", "grp"),
        P("wide", "grp"),
        P(),
    )
    out_specs = (P(None, "wide", "grp"), P("wide", "grp"))
    return jax.shard_map(
        per_device, mesh=mesh, in_specs=in_specs, out_specs=out_specs, check_vma=False
    )
```

```python
import functools

import jax
import jax.numpy as jnp
from jax import lax
from jax.experimental import pallas as pl
from jax.experimental.pallas import tpu as pltpu
from jax.sharding import PartitionSpec as P

MESH = pl.DeviceIdType.MESH
BF16 = jnp.bfloat16
F32 = jnp.float32
COPIES = 103
SENDS = 24
LOCALS = 8
TILE = 256


def dot_nt(a, b):
    return lax.dot_general(a, b, (((1,), (1,)), ((), ())), preferred_element_type=F32)


def dot_nn(a, b):
    return lax.dot_general(a, b, (((1,), (0,)), ((), ())), preferred_element_type=F32)


def split_columns(quarter):
    tiles = quarter // TILE
    low = max(1, 3 * tiles // 7)
    return low * TILE, (tiles - low) * TILE


class Wire:
    def __init__(self, send_sems, recv_sems):
        self.send_sems, self.recv_sems = send_sems, recv_sems
        self.count = 0
        self.sent = []

    def send(self, src, dst, device):
        lane = self.count % SENDS
        if self.count >= SENDS:
            self.sent[self.count - SENDS].wait_send()
        copy = pltpu.make_async_remote_copy(
            src_ref=src,
            dst_ref=dst,
            send_sem=self.send_sems.at[lane],
            recv_sem=self.recv_sems.at[self.count],
            device_id=device,
            device_id_type=MESH,
        )
        self.count += 1
        copy.start()
        self.sent.append(copy)
        return copy

    def drain(self):
        for copy in self.sent[-SENDS:]:
            copy.wait_send()


def kernel(
    pool, ids, cot, gate_up, down, exponent,
    out_pair, out_down,
    tok_x, tok_c, via_x, via_c, picked, pool_q, weights,
    part, part_own, r1p, r1m, r2p, r2m, deltas, grads,
    ring_a, sum_a, ya1p, ya1m, ya2p, ya2m,
    yb1p, yb1m, yb2p, yb2m, sum_b, ring_b,
    final, crossed, ids_v, send_sems, recv_sems, local_sems,
):
    tokens, width = cot.shape
    quarter = width // 4
    half = quarter // 2
    own_rows = down.shape[0]
    pair_rows = 2 * own_rows
    chunk_rows = 4 * pair_rows
    chip_tokens = 2 * tokens
    pool_rows = pool.shape[0]
    tile = TILE
    part_a, part_b = split_columns(quarter)

    x_lo = lax.axis_index("grp")
    wide = lax.axis_index("wide")
    z = lax.div(wide, 16)
    x_hi = lax.rem(lax.div(wide, 8), 2)
    y = lax.rem(lax.div(wide, 2), 4)
    core = lax.rem(wide, 2)
    x = 2 * x_hi + x_lo
    device_index = x_lo * 64 + wide

    def shift(v, by):
        return lax.rem(v + (by % 4), 4)

    def device(xx, yy, zz, cc):
        return (lax.rem(xx, 2), zz * 16 + lax.div(xx, 2) * 8 + yy * 2 + cc)

    xn, xf, xb = shift(x, 1), shift(x, 2), shift(x, -1)
    yn, yf, yb = shift(y, 1), shift(y, 2), shift(y, -1)
    zn, zf, zb = shift(z, 1), shift(z, 2), shift(z, -1)
    z_on, z_off = (lax.rem(z + 4 + s, 4) for s in (1 - 2 * core, 2 * core - 1))
    x_next, x_far, x_back = (device(v, y, z, core) for v in (xn, xf, xb))
    y_next, y_back = (device(x, v, z, core) for v in (yn, yb))
    z_next, z_back = (device(x, y, v, core) for v in (zn, zb))
    z_ring = device(x, y, z_on, core)
    partner = device(x, y, z, 1 - core)

    def feature_quarter(xx):
        return 2 * lax.rem(xx, 2) + lax.div(xx, 2)

    def q_cols(xx):
        return pl.ds(pl.multiple_of(feature_quarter(xx) * quarter, quarter), quarter)

    def slot(xx, cc):
        return pl.ds(pl.multiple_of((2 * xx + cc) * tokens, tokens), tokens)

    def chip_slot(xx):
        return pl.ds(pl.multiple_of(xx * chip_tokens, chip_tokens), chip_tokens)

    def rows_of(yy):
        return pl.ds(pl.multiple_of(yy * pair_rows, pair_rows), pair_rows)

    def low_rows_of(yy):
        return pl.ds(pl.multiple_of(yy * pair_rows, own_rows), own_rows)

    def high_rows_of(yy):
        return pl.ds(pl.multiple_of(yy * pair_rows + own_rows, own_rows), own_rows)

    def owner_rows(xh):
        return pl.ds(pl.multiple_of(y * pair_rows + xh * own_rows, own_rows), own_rows)

    cols_a = pl.ds(0, half)
    cols_b = pl.ds(half, half)
    all_p = pl.ds(0, 3)
    wire = Wire(send_sems, recv_sems)
    locals_used = [0]

    def fetch(src, dst):
        copy = pltpu.make_async_copy(src, dst, local_sems.at[locals_used[0]])
        locals_used[0] += 1
        copy.start()
        return copy

    ids_here = fetch(ids, ids_v)
    far_pool = fetch(pool.at[:, q_cols(xf)], pool_q.at[0])

    barrier = pltpu.get_barrier_semaphore()
    for peer in (x_next, x_back, x_far, y_next, y_back, z_next, z_back, partner):
        pl.semaphore_signal(barrier, inc=1, device_id=peer, device_id_type=MESH)
    pl.semaphore_wait(barrier, 8)

    x_hi_cols = pl.ds(pl.multiple_of(x_hi * quarter, quarter), quarter)
    other_cols = pl.ds(pl.multiple_of((1 - x_hi) * quarter, quarter), quarter)
    wx_pair = wire.send(
        gate_up.at[:, :, other_cols], weights.at[z, pl.ds(0, 2), owner_rows(x_hi), :], x_far
    )
    wx_down = wire.send(down.at[:, other_cols], weights.at[z, 2, owner_rows(x_hi), :], x_far)
    w_pair = fetch(gate_up.at[:, :, x_hi_cols], weights.at[z, pl.ds(0, 2), owner_rows(x_hi), :])
    w_down = fetch(down.at[:, x_hi_cols], weights.at[z, 2, owner_rows(x_hi), :])

    c_via = wire.send(cot.at[:, q_cols(xf)], via_c, x_back)
    early, late = pl.ds(0, tokens // 2), pl.ds(tokens // 2, tokens // 2)

    def half_slot(part_index):
        start = (2 * x + core) * tokens + part_index * (tokens // 2)
        return pl.ds(pl.multiple_of(start, tokens // 2), tokens // 2)

    c_next_a = wire.send(cot.at[early, q_cols(xn)], tok_c.at[half_slot(0), :], x_next)
    c_back = wire.send(cot.at[:, q_cols(xb)], tok_c.at[slot(x, core), :], x_back)
    c_own = fetch(cot.at[:, q_cols(x)], tok_c.at[slot(x, core), :])
    next_pool = fetch(pool.at[:, q_cols(xn)], pool_q.at[1])
    back_pool = fetch(pool.at[:, q_cols(xb)], pool_q.at[2])
    own_pool = fetch(pool.at[:, q_cols(x)], pool_q.at[3])

    ids_here.wait()
    local_ids = ids_v[...] - device_index * pool_rows
    row_ids = lax.broadcasted_iota(jnp.int32, (pool_rows, tokens), 0)
    chosen = jnp.where(row_ids == local_ids, 1.0, 0.0).astype(F32).T.astype(BF16)

    def pick(index, target, row_slot):
        def step(n, carry):
            cols = pl.ds(pl.multiple_of(n * tile, tile), tile)
            target[row_slot, cols] = dot_nn(chosen, pool_q[index, :, cols]).astype(BF16)
            return carry

        lax.fori_loop(0, quarter // tile, step, 0)

    every = pl.ds(0, tokens)
    far_pool.wait()
    pick(0, picked.at[0], every)
    x_via = wire.send(picked.at[0], via_x, x_next)
    c_next_b = wire.send(cot.at[late, q_cols(xn)], tok_c.at[half_slot(1), :], x_next)

    w_pair.wait()
    w_down.wait()
    wx_pair.wait_recv()
    wx_down.wait_recv()

    def w_block(zz, rows, cols):
        return weights.at[zz, all_p, rows, cols]

    def same(view, device_):
        return wire.send(view, view, device_)

    a_next = same(w_block(z, rows_of(y), cols_a), y_next)
    a_back = same(w_block(z, rows_of(y), cols_a), y_back)
    b_next = same(w_block(z, rows_of(y), cols_b), z_next)
    b_back = same(w_block(z, rows_of(y), cols_b), z_back)


    a_next.wait_recv()
    a_on = same(w_block(z, low_rows_of(yb), cols_a), y_next)
    a_back.wait_recv()
    a_off = same(w_block(z, high_rows_of(yn), cols_a), y_back)
    b_next.wait_recv()
    b_on = same(w_block(zb, low_rows_of(y), cols_b), z_next)
    b_back.wait_recv()
    b_off = same(w_block(zn, high_rows_of(y), cols_b), z_back)

    next_pool.wait()
    pick(1, picked.at[1], every)
    back_pool.wait()
    pick(2, picked.at[2], every)

    a_on.wait_recv()
    a_off.wait_recv()
    every_row = pl.ds(0, chunk_rows)
    lower, upper = pl.ds(0, chunk_rows // 2), pl.ds(chunk_rows // 2, chunk_rows // 2)
    a2_next = same(w_block(z, every_row, cols_a), z_next)
    a2_back = same(w_block(z, every_row, cols_a), z_back)
    b_on.wait_recv()
    b_off.wait_recv()
    b2_next = same(w_block(pl.ds(0, 4), rows_of(y), cols_b), y_next)
    b2_back = same(w_block(pl.ds(0, 4), rows_of(y), cols_b), y_back)

    c_via.wait_recv()
    c_pass = wire.send(via_c, tok_c.at[slot(xn, core), :], x_back)
    x_back_copy = wire.send(picked.at[2], tok_x.at[slot(x, core), :], x_back)
    x_via.wait_recv()
    x_pass = wire.send(via_x, tok_x.at[slot(xb, core), :], x_next)
    x_next_copy = wire.send(picked.at[1], tok_x.at[slot(x, core), :], x_next)

    own_pool.wait()
    pick(3, tok_x, slot(x, core))
    dd_own_x = same(tok_x.at[slot(x, core), :], partner)
    c_own.wait()
    dd_own_c = same(tok_c.at[slot(x, core), :], partner)
    c_back.wait_recv()
    dd_c_n = same(tok_c.at[slot(xn, core), :], partner)
    c_next_a.wait_recv()
    c_next_b.wait_recv()
    dd_c_b = same(tok_c.at[slot(xb, core), :], partner)

    a2_next.wait_recv()
    a2_on = same(w_block(zb, lower, cols_a), z_next)
    a2_back.wait_recv()
    a2_off = same(w_block(zn, upper, cols_a), z_back)
    b2_next.wait_recv()
    b2_on = same(w_block(pl.ds(0, 2), rows_of(yb), cols_b), y_next)
    b2_back.wait_recv()
    b2_off = same(w_block(pl.ds(2, 2), rows_of(yn), cols_b), y_back)

    c_pass.wait_recv()
    dd_c_f = same(tok_c.at[slot(xf, core), :], partner)
    x_pass.wait_recv()
    dd_x_f = same(tok_x.at[slot(xf, core), :], partner)

    for copy in (a2_on, a2_off, b2_on, b2_off):
        copy.wait_recv()

    def forward(xx, target):
        def step(j, carry):
            tx = tok_x[chip_slot(xx), :]
            for h in range(2):
                pair = weights[2 * j + h, 0:2].reshape(2 * chunk_rows, quarter)
                target[2 * j + h, :, 0 : 2 * chunk_rows] = dot_nt(tx, pair).astype(target.dtype)
            tc = tok_c[chip_slot(xx), :]
            both = weights[pl.ds(2 * j, 2), 2].reshape(2 * chunk_rows, quarter)
            back = dot_nt(tc, both).astype(target.dtype)
            target[2 * j, :, 2 * chunk_rows :] = back[:, :chunk_rows]
            target[2 * j + 1, :, 2 * chunk_rows :] = back[:, chunk_rows:]
            return carry

        lax.fori_loop(0, 2, step, 0)

    first, second = pl.ds(0, tokens), pl.ds(tokens, tokens)
    dd_c_f.wait_recv()
    dd_x_f.wait_recv()
    forward(xf, part.at[xf])
    order = (z_off, zf, z_on, z)
    rs1 = []
    for zz in order:
        rs1.append(
            (
                wire.send(part.at[xf, zz, first, :], r1p.at[zz], x_next),
                wire.send(part.at[xf, zz, second, :], r1m.at[zz], x_back),
            )
        )
    dd_own_x.wait_recv()
    dd_own_c.wait_recv()
    forward(x, part_own)

    x_back_copy.wait_recv()
    dd_x_n = same(tok_x.at[slot(xn, core), :], partner)
    x_next_copy.wait_recv()
    dd_x_b = same(tok_x.at[slot(xb, core), :], partner)
    dd_c_n.wait_recv()
    dd_x_n.wait_recv()
    forward(xn, part.at[xn])
    dd_c_b.wait_recv()
    dd_x_b.wait_recv()
    forward(xb, part.at[xb])

    def add_into(ref, *others):
        total = ref[...].astype(F32)
        for other in others:
            total = total + other[...].astype(F32)
        ref[...] = total.astype(ref.dtype)

    def own_lanes(xx):
        return pl.ds(pl.multiple_of(xx * chip_tokens, chip_tokens), chip_tokens)

    def low_lanes(xx):
        return pl.ds(pl.multiple_of(xx * chip_tokens, tokens), tokens)

    def high_lanes(xx):
        return pl.ds(pl.multiple_of(xx * chip_tokens + tokens, tokens), tokens)

    level = exponent[0]
    unscale = jnp.float32(0.0)
    for power in range(16):
        unscale = jnp.where(level == power, jnp.float32(0.5**power), unscale)

    every_unit = pl.ds(0, chunk_rows)
    rs2, ag, passed, yb1, yb2 = {}, {}, {}, {}, {}

    def reduce_on(k):
        zz = order[k]
        rs1[k][0].wait_recv()
        add_into(part.at[xn, zz, first, :], r1p.at[zz])
        fwd = wire.send(part.at[xn, zz], r2p.at[zz], x_next)
        rs1[k][1].wait_recv()
        add_into(part.at[xb, zz, second, :], r1m.at[zz])
        rs2[k] = (fwd, wire.send(part.at[xb, zz], r2m.at[zz], x_back))

    def activate(k):
        zz = order[k]
        rs2[k][0].wait_recv()
        rs2[k][1].wait_recv()
        total = part_own[zz] + r2p[zz].astype(F32) + r2m[zz].astype(F32)
        gate = total[:, :chunk_rows]
        up = total[:, chunk_rows : 2 * chunk_rows]
        delta = unscale * total[:, 2 * chunk_rows :]
        sig = 1.0 / (1.0 + jnp.exp(-gate))
        hidden = gate * sig * up
        delta_gate = delta * up * sig * (1.0 + gate * (1.0 - sig))
        delta_up = delta * gate * sig
        deltas[zz, 0, :, own_lanes(x)] = delta_gate.T.astype(BF16)
        deltas[zz, 1, :, own_lanes(x)] = delta_up.T.astype(BF16)
        deltas[zz, 2, :, own_lanes(x)] = hidden.T.astype(BF16)

    def gather(k):
        zz = order[k]
        low = deltas.at[zz, all_p, every_unit, low_lanes(x)]
        high = deltas.at[zz, all_p, every_unit, high_lanes(x)]
        early = (same(low, x_next), same(high, x_back))
        ag[k] = (early, (same(high, x_next), same(low, x_back)))

    def pass_on(k):
        zz = order[k]
        ag[k][0][0].wait_recv()
        on = same(deltas.at[zz, all_p, every_unit, low_lanes(xb)], x_next)
        ag[k][0][1].wait_recv()
        passed[k] = (on, same(deltas.at[zz, all_p, every_unit, high_lanes(xn)], x_back))

    def gathered(k):
        ag[k][1][0].wait_recv()
        ag[k][1][1].wait_recv()
        passed[k][0].wait_recv()
        passed[k][1].wait_recv()

    def grad_half(k, start, size):
        zz = order[k]

        def step(n, carry):
            cols = pl.ds(pl.multiple_of(start + n * tile, tile), tile)
            pair = deltas[zz, 0:2].reshape(2 * chunk_rows, 4 * chip_tokens)
            out = dot_nn(pair, tok_x[:, cols]).astype(BF16)
            grads[zz, 0, :, cols] = out[:chunk_rows]
            grads[zz, 1, :, cols] = out[chunk_rows:]
            down_part = unscale * dot_nn(deltas[zz, 2], tok_c[:, cols])
            grads[zz, 2, :, cols] = down_part.astype(BF16)
            return carry

        lax.fori_loop(0, size // tile, step, 0)

    cols_a, cols_b = pl.ds(0, part_a), pl.ds(part_a, part_b)

    def g_block(zz, rows, cols):
        return grads.at[zz, all_p, rows, cols]

    def add3(out, *terms):
        for p in range(3):
            total = terms[0][p].astype(F32)
            for term in terms[1:]:
                total = total + term[p].astype(F32)
            out[p] = total.astype(out.dtype)

    ring_of_a, ring_of_b = [], []

    def a_step(k):
        view = g_block(order[k], every_row, cols_a)
        if k > 0:
            ring_of_a[k - 1].wait_recv()
            add3(view, view, ring_a.at[k - 1])
        ring_of_a.append(wire.send(view, ring_a.at[k], z_ring))

    def b_step(k):
        view = sum_b.at[order[k]]
        if k > 0:
            ring_of_b[k - 1].wait_recv()
            add3(view, view, ring_b.at[k - 1])
        ring_of_b.append(wire.send(view, ring_b.at[k], z_ring))

    def b_first(k):
        zz = order[k]
        yb1[k] = (
            wire.send(g_block(zz, low_rows_of(yf), cols_b), yb1p.at[zz], y_next),
            wire.send(g_block(zz, high_rows_of(yf), cols_b), yb1m.at[zz], y_back),
        )

    def b_second(k):
        zz = order[k]
        yb1[k][0].wait_recv()
        view = g_block(zz, low_rows_of(yn), cols_b)
        add3(view, view, yb1p.at[zz])
        on = wire.send(g_block(zz, rows_of(yn), cols_b), yb2p.at[zz], y_next)
        yb1[k][1].wait_recv()
        view = g_block(zz, high_rows_of(yb), cols_b)
        add3(view, view, yb1m.at[zz])
        yb2[k] = (on, wire.send(g_block(zz, rows_of(yb), cols_b), yb2m.at[zz], y_back))

    def b_sum(k):
        zz = order[k]
        yb2[k][0].wait_recv()
        yb2[k][1].wait_recv()
        add3(sum_b.at[zz], g_block(zz, rows_of(y), cols_b), yb2p.at[zz], yb2m.at[zz])

    reduce_on(0)
    reduce_on(1)
    activate(0)
    gather(0)
    reduce_on(2)
    activate(1)
    pass_on(0)
    gather(1)
    reduce_on(3)
    activate(2)

    gathered(0)
    grad_half(0, 0, part_a)
    a_step(0)
    pass_on(1)
    gather(2)
    grad_half(0, part_a, part_b)
    b_first(0)
    b_second(0)
    activate(3)

    gathered(1)
    grad_half(1, 0, part_a)
    a_step(1)
    pass_on(2)
    gather(3)
    grad_half(1, part_a, part_b)
    b_first(1)
    b_sum(0)
    b_step(0)

    gathered(2)
    grad_half(2, 0, part_a)
    b_second(1)
    pass_on(3)
    grad_half(2, part_a, part_b)
    b_first(2)
    a_step(2)

    gathered(3)
    grad_half(3, part_a, part_b)
    b_first(3)
    b_second(2)
    grad_half(3, 0, part_a)
    b_sum(1)
    b_step(1)
    ring_of_a[2].wait_recv()
    add3(sum_a, g_block(z, every_row, cols_a), ring_a.at[2])

    def a_block(rows):
        return sum_a.at[all_p, rows, :]

    ya1 = (
        wire.send(a_block(low_rows_of(yf)), ya1p, y_next),
        wire.send(a_block(high_rows_of(yf)), ya1m, y_back),
    )
    b_second(3)
    b_sum(2)
    b_step(2)
    ya1[0].wait_recv()
    view = a_block(low_rows_of(yn))
    add3(view, view, ya1p)
    ya2_next = wire.send(a_block(rows_of(yn)), ya2p, y_next)
    ya1[1].wait_recv()
    view = a_block(high_rows_of(yb))
    add3(view, view, ya1m)
    ya2_back = wire.send(a_block(rows_of(yb)), ya2m, y_back)
    b_sum(3)
    ring_of_b[2].wait_recv()
    every_pair = pl.ds(0, pair_rows)
    add3(final.at[all_p, every_pair, cols_b], sum_b.at[z], ring_b.at[2])
    kept = pl.ds(pl.multiple_of(x_hi * own_rows, own_rows), own_rows)
    given = pl.ds(pl.multiple_of((1 - x_hi) * own_rows, own_rows), own_rows)
    every_own = pl.ds(0, own_rows)
    last_b = wire.send(
        final.at[all_p, given, cols_b], crossed.at[all_p, every_own, cols_b], x_far
    )
    ya2_next.wait_recv()
    ya2_back.wait_recv()
    add3(final.at[all_p, every_pair, cols_a], a_block(rows_of(y)), ya2p, ya2m)
    last_a = wire.send(
        final.at[all_p, given, cols_a], crossed.at[all_p, every_own, cols_a], x_far
    )
    out_pair[:, :, x_hi_cols] = final[0:2, kept, :]
    out_down[:, x_hi_cols] = final[2, kept, :]
    last_b.wait_recv()
    last_a.wait_recv()
    out_pair[:, :, other_cols] = crossed[0:2]
    out_down[:, other_cols] = crossed[2]
    wire.drain()


def per_device(x_pool, token_ids, cotangent, gate_up, down_weight, loss_exponent):
    tokens, width = cotangent.shape
    quarter = width // 4
    half = quarter // 2
    own_rows = down_weight.shape[0]
    pair_rows, chunk_rows = 2 * own_rows, 8 * own_rows
    chip_tokens, ring_tokens = 2 * tokens, 8 * tokens
    acts = 3 * chunk_rows
    part_a, part_b = split_columns(quarter)

    def held(*shape, dtype=BF16):
        return pltpu.VMEM(shape, dtype)

    scratch = [
        held(ring_tokens, quarter), held(ring_tokens, quarter),
        held(tokens, quarter), held(tokens, quarter),
        held(3, tokens, quarter), held(4, x_pool.shape[0], quarter),
        held(4, 3, chunk_rows, quarter),
        held(4, 4, chip_tokens, acts), held(4, chip_tokens, acts, dtype=F32),
        held(4, tokens, acts), held(4, tokens, acts),
        held(4, chip_tokens, acts), held(4, chip_tokens, acts),
        held(4, 3, chunk_rows, ring_tokens),
        held(4, 3, chunk_rows, quarter),
        held(3, 3, chunk_rows, part_a), held(3, chunk_rows, part_a),
        held(3, own_rows, part_a), held(3, own_rows, part_a),
        held(3, pair_rows, part_a), held(3, pair_rows, part_a),
        held(4, 3, own_rows, part_b), held(4, 3, own_rows, part_b),
        held(4, 3, pair_rows, part_b), held(4, 3, pair_rows, part_b),
        held(4, 3, pair_rows, part_b), held(3, 3, pair_rows, part_b),
        held(3, pair_rows, quarter), held(3, own_rows, quarter),
        pltpu.VMEM((1, tokens), jnp.int32),
        pltpu.SemaphoreType.DMA((SENDS,)),
        pltpu.SemaphoreType.DMA((COPIES,)),
        pltpu.SemaphoreType.DMA((LOCALS,)),
    ]
    far = pl.BlockSpec(memory_space=pltpu.HBM)
    near = pl.BlockSpec(memory_space=pltpu.VMEM)
    return pl.pallas_call(
        kernel,
        out_shape=(
            jax.ShapeDtypeStruct(gate_up.shape, BF16),
            jax.ShapeDtypeStruct(down_weight.shape, BF16),
        ),
        in_specs=[far, far, far, far, far, pl.BlockSpec(memory_space=pltpu.SMEM)],
        out_specs=(near, near),
        scratch_shapes=scratch,
        compiler_params=pltpu.CompilerParams(
            collective_id=0, has_side_effects=True, vmem_limit_bytes=56_000_000
        ),
    )(*[pltpu.with_memory_space_constraint(v, pltpu.HBM) for v in (x_pool, token_ids.reshape(1, tokens), cotangent, gate_up, down_weight)], loss_exponent)


def solution(mesh):
    in_specs = (
        P(("grp", "wide"), None),
        P(("grp", "wide")),
        P(("grp", "wide"), None),
        P(None, "wide", "grp"),
        P("wide", "grp"),
        P(),
    )
    out_specs = (P(None, "wide", "grp"), P("wide", "grp"))
    return jax.shard_map(
        per_device, mesh=mesh, in_specs=in_specs, out_specs=out_specs, check_vma=False
    )
```
